32 devices in a mesh: aper: 4 (over y, x), rng: 4 (over z), beam: 2 (over core).
Axes of the slice: x: 2, y: 2, z: 4, core: 2. Of those that a mesh axis runs over, the one named last changes fastest.
Arguments:
- children: float32 [4, 2, 8192, 256], P('aper', None, 'rng', 'beam'), may hold values from -6 to 6
- shift_one: int32 [2, 256], replicated, may hold values from -8 to 8
- rtaps_one: float32 [2, 8, 256], replicated, may hold values from -2 to 2
- bstart_one: int32 [2, 512], replicated, may hold values from -5 to 252, as said below
- btaps_one: float32 [2, 8, 512], replicated, may hold values from -2 to 2
- prate_one: float32 [2, 512], replicated, may hold values from -64 to 64
- poff_one: float32 [2, 512], replicated, may hold values from -3.140625 to 3.140625
- shift_two: int32 [2, 512], replicated, may hold values from -8 to 8
- rtaps_two: float32 [2, 8, 512], replicated, may hold values from -2 to 2
- bstart_two: int32 [2, 1024], replicated, may hold values from -5 to 508, as said below
- btaps_two: float32 [2, 8, 1024], replicated, may hold values from -2 to 2
- prate_two: float32 [2, 1024], replicated, may hold values from -64 to 64
- poff_two: float32 [2, 1024], replicated, may hold values from -3.140625 to 3.140625
Outputs:
- merged: float32 [4, 2, 8192, 256], P('aper', None, 'rng', 'beam')
The draws below stay inside these ranges and needn't reach their ends.
Inputs may be any that keep to these rules, and one draw needn't show every extreme that they name: bstart_one[c, b] is b // 2 - 8 // 2 plus -1, 0 or 1. bstart_two[c, b] is b // 2 - 8 // 2 plus -1, 0 or 1.
All inputs are finite; a program needn't handle non-finite values.
Results may differ from the reference program's by a relative error of at most 0.0003.
Values sent between devices are 32-bit elements; how exact they have to be, the bound alone decides.
No kernel may reach another device: no remote copies, remote signals or barrier semaphores. Data moves between devices by JAX's collectives and lax.ppermute only.
A program may use at most 64 MiB of HBM per device.

```python
import jax
import jax.numpy as jnp
from jax import lax

BEAMS = 256
RTAPS = 8
BTAPS = 8
SHIFT = 8
RRIM = 12
RANGE = 8192
SUBAPS = 4
N_BEAM = 2


def draw_bstart_one(key, part):
    base_rows = jnp.arange(2 * BEAMS, dtype=jnp.int32) // 2 - BTAPS // 2
    jitter = jax.random.randint(jax.random.fold_in(key, 11), (2, 2 * BEAMS), -1, 2)
    return (base_rows[None, :] + jitter).astype(jnp.int32)


def draw_bstart_two(key, part):
    base_rows = jnp.arange(4 * BEAMS, dtype=jnp.int32) // 2 - BTAPS // 2
    jitter = jax.random.randint(jax.random.fold_in(key, 23), (2, 4 * BEAMS), -1, 2)
    return (base_rows[None, :] + jitter).astype(jnp.int32)


def with_ends(drawn, rng, least, largest):
    longest = drawn.shape.index(max(drawn.shape))
    spots = []
    for shift in (0, 1):
        where = [jax.random.randint(jax.random.fold_in(rng, axis), (), 0, length) for axis, length in enumerate(drawn.shape)]
        where[longest] = (where[longest] + shift) % drawn.shape[longest]
        spots.append(tuple(where))
    return drawn.at[spots[0]].set(least).at[spots[1]].set(largest)


def block_scale(key, extent, shards, least, high):
    def one(position, shards_of):
        heights = jax.random.uniform(jax.random.fold_in(jax.random.fold_in(key, 6), position), (shards_of,), jnp.float32, least / len(shards), high / len(shards))
        return jnp.repeat(jnp.exp(heights), extent[position] // shards_of).reshape((-1,) + (1,) * (len(extent) - position - 1))

    loudness = one(*shards[0])
    for cut in shards[1:]:
        loudness = loudness * one(*cut)
    return loudness


def bell_draw(key, shape, scale, most, split=(), held_as=jnp.bfloat16):
    drawn = jax.random.normal(key, shape, jnp.float32) * scale
    if len(split) > 0:
        drawn = block_scale(key, shape, split, -0.22, 0.18) * drawn
    return jnp.clip(drawn, min=-most, max=most).astype(held_as)


def setup_inputs(seed: int = 0) -> dict:
    seeds = jax.random.split(jax.random.key(seed), 14)
    return {
        "children": bell_draw(seeds[0], (SUBAPS, 2, RANGE, BEAMS), 1.0, 6.0, ((0, 4), (2, 4), (3, 2)), jnp.float32),
        "shift_one": with_ends(jax.random.randint(seeds[1], (2, BEAMS), -SHIFT, SHIFT + 1), jax.random.fold_in(seeds[1], 1), -SHIFT, SHIFT).astype(jnp.int32),
        "rtaps_one": bell_draw(seeds[2], (2, RTAPS, BEAMS), RTAPS ** -0.5, 2.0, (), jnp.float32),
        "bstart_one": draw_bstart_one(jax.random.fold_in(seeds[13], 71), 0),
        "btaps_one": bell_draw(seeds[4], (2, BTAPS, 2 * BEAMS), BTAPS ** -0.5, 2.0, (), jnp.float32),
        "prate_one": jnp.clip(jax.random.uniform(seeds[5], (2, 2 * BEAMS), jnp.float32, -64.0, 64.0), -64.0, 64.0),
        "poff_one": jnp.clip(jax.random.uniform(seeds[6], (2, 2 * BEAMS), jnp.float32, -3.140625, 3.140625), -3.140625, 3.140625),
        "shift_two": with_ends(jax.random.randint(seeds[7], (2, 2 * BEAMS), -SHIFT, SHIFT + 1), jax.random.fold_in(seeds[7], 1), -SHIFT, SHIFT).astype(jnp.int32),
        "rtaps_two": bell_draw(seeds[8], (2, RTAPS, 2 * BEAMS), RTAPS ** -0.5, 2.0, (), jnp.float32),
        "bstart_two": draw_bstart_two(jax.random.fold_in(seeds[13], 71), 0),
        "btaps_two": bell_draw(seeds[10], (2, BTAPS, 4 * BEAMS), BTAPS ** -0.5, 2.0, (), jnp.float32),
        "prate_two": jnp.clip(jax.random.uniform(seeds[11], (2, 4 * BEAMS), jnp.float32, -64.0, 64.0), -64.0, 64.0),
        "poff_two": jnp.clip(jax.random.uniform(seeds[12], (2, 4 * BEAMS), jnp.float32, -3.140625, 3.140625), -3.140625, 3.140625),
    }


def range_interp(child_image, shifts, weights):
    rows_all = child_image.shape[1]
    padded = jnp.pad(child_image, ((0, 0), (RRIM, RRIM), (0, 0)))
    base_rows = jnp.arange(rows_all, dtype=jnp.int32)[:, None] + RRIM + shifts.astype(jnp.int32)[None, :]
    summed = jnp.zeros(child_image.shape, jnp.float32)
    for tap_index in range(RTAPS):
        row_index = jnp.broadcast_to((base_rows + (tap_index - RTAPS // 2)).astype(jnp.int32)[None], child_image.shape)
        summed = summed + weights[tap_index][None, None, :] * jnp.take_along_axis(padded, row_index, axis=1)
    return summed


def beam_interp(level_vals, starts, weights, rates, offsets, range_frac):
    ext_width = level_vals.shape[2]
    col_count = starts.shape[0]
    column_ids = lax.broadcasted_iota(jnp.int32, (ext_width, col_count, BTAPS), 0)
    taps_at = starts.astype(jnp.int32)[None, :, None] + lax.broadcasted_iota(jnp.int32, (ext_width, col_count, BTAPS), 2)
    matrix = jnp.sum(jnp.where(column_ids == taps_at, jnp.transpose(weights)[None], jnp.zeros((), jnp.float32)), axis=2)
    rows_all = level_vals.shape[1]
    mixed_vals = jnp.dot(level_vals.reshape(2 * rows_all, ext_width), matrix, precision=lax.Precision.HIGHEST, preferred_element_type=jnp.float32).reshape(2, rows_all, col_count)
    phase_angle = range_frac[:, None] * rates[None, :] + offsets[None, :]
    cosine = jnp.cos(phase_angle)
    sine_part = jnp.sin(phase_angle)
    return jnp.stack([cosine * mixed_vals[0] - sine_part * mixed_vals[1], sine_part * mixed_vals[0] + cosine * mixed_vals[1]])


def merge_ref(left_image, right_image, tables, range_frac):
    shift_tab, rtap_tab, start_tab, btap_tab, rate_tab, off_tab = tables
    summed = None
    for side_index, child_image in ((0, left_image), (1, right_image)):
        level_vals = range_interp(child_image, shift_tab[side_index], rtap_tab[side_index])
        term = beam_interp(level_vals, start_tab[side_index], btap_tab[side_index], rate_tab[side_index], off_tab[side_index], range_frac)
        summed = term if summed is None else summed + term
    return summed


def reference(children, shift_one, rtaps_one, bstart_one, btaps_one, prate_one, poff_one, shift_two, rtaps_two, bstart_two, btaps_two, prate_two, poff_two):
    rows_all = children.shape[2]
    range_frac = jnp.arange(rows_all, dtype=jnp.int32).astype(jnp.float32) / rows_all
    tables_one = (shift_one, rtaps_one, bstart_one, btaps_one, prate_one, poff_one)
    tables_two = (shift_two, rtaps_two, bstart_two, btaps_two, prate_two, poff_two)
    group_count = children.shape[0] // 4
    groups = children.reshape(group_count, 4, 2, rows_all, BEAMS)

    def one_group(quartet):
        left_parent = merge_ref(quartet[0], quartet[2], tables_one, range_frac)
        right_parent = merge_ref(quartet[1], quartet[3], tables_one, range_frac)
        return merge_ref(left_parent, right_parent, tables_two, range_frac)

    finals = lax.map(one_group, groups)
    beam_block = BEAMS // N_BEAM
    shaped = finals.reshape(group_count, 2, rows_all, N_BEAM, 4, beam_block)
    shaped = jnp.transpose(shaped, (0, 4, 1, 2, 3, 5))
    return shaped.reshape(group_count * 4, 2, rows_all, BEAMS)
```

```python
import functools

import jax
import jax.numpy as jnp
from jax import lax
from jax.experimental import pallas as pl
from jax.experimental.pallas import tpu as pltpu
from jax.sharding import PartitionSpec as P

TAPS = 8
SPAN = 8
GROUP = 4
TILE = 128
RIM = 8
PRIM = 5
HALO = 16
FINE = 2 * TAPS - 1
ANY = pl.BlockSpec(memory_space=pl.ANY)
SMEM = pl.BlockSpec(memory_space=pltpu.SMEM)
VMEM = pl.BlockSpec(memory_space=pltpu.VMEM)
F32 = jnp.float32
BF16 = jnp.bfloat16


def plan_of(tiles):
    quarter = tiles // 4
    half = quarter // 2
    ring = list(range(tiles - half, tiles)) + list(range(tiles - half))
    return [ring[i * quarter : (i + 1) * quarter] for i in range(4)]


def spans(tiles):
    runs = []
    for position, tile in enumerate(tiles):
        if runs and tile == runs[-1][1] + runs[-1][2]:
            runs[-1][2] += 1
        else:
            runs.append([position, tile, 1])
    return runs


def lanes(tile, count=1):
    return pl.ds(tile * TILE, count * TILE)


def run_copies(copies):
    for copy in copies:
        copy.start()
    for copy in copies:
        copy.wait()


def first_pack(plan, sc, child, *refs):
    outs, (rim, flat, rows_in, turned, in_sem, out_sem, flat_sem) = refs[:3], refs[3:]
    blk = child.shape[3]
    sub = blk // GROUP
    tiles = child.shape[2] // TILE
    mine = sc[0]
    edge = spans(plan[0])
    rest = [[0, plan[1][0], tiles - len(plan[0])]]

    def fetch(part, sem):
        return [
            pltpu.make_async_copy(
                child.at[0, :, lanes(first, count), :], rows_in.at[:, lanes(first, count), :], sem
            )
            for _, first, count in part
        ]

    early = fetch(edge, in_sem.at[0])
    late = fetch(rest, in_sem.at[1])
    for copy in early + late:
        copy.start()

    def turn(tile):
        for part in range(2):
            turned[part, :, lanes(tile)] = rows_in[part, lanes(tile), :].T

    for copy in early:
        copy.wait()
    for tile in plan[0]:
        turn(tile)
    sends = []
    for k in range(1, GROUP):
        other = jnp.bitwise_xor(mine, k)
        beams = pl.ds(pl.multiple_of(other * sub, 8), sub)
        for position, first, count in edge:
            sends.append(
                pltpu.make_async_copy(
                    turned.at[:, beams, lanes(first, count)],
                    outs[k - 1].at[:, :, lanes(position, count)],
                    out_sem,
                )
            )
    for copy in sends:
        copy.start()
    for copy in late:
        copy.wait()
    first, count = rest[0][1], rest[0][2]

    def step(i, carry):
        for j in range(2):
            turn(first + 2 * i + j)
        return carry

    lax.fori_loop(0, count // 2, step, 0)
    side = pl.ds(pl.multiple_of((1 - sc[1]) * (blk - RIM), 8), RIM)
    tail = [
        pltpu.make_async_copy(turned, flat, flat_sem),
        pltpu.make_async_copy(turned.at[:, side, :], rim, flat_sem),
    ]
    run_copies(tail)
    for copy in sends:
        copy.wait()


def second_pack(plan, sc, flat, rim, *refs):
    outs, (own, turned, in_sem, out_sem) = refs[:9], refs[9:]
    blk = flat.shape[1]
    sub = blk // GROUP
    mine, beam = sc[0], sc[1]
    wide = sub + 2 * RIM
    low, high = pl.ds(0, RIM), pl.ds(RIM + blk, RIM)
    load = pltpu.make_async_copy(flat, turned.at[:, pl.ds(RIM, blk), :], in_sem.at[0])
    load.start()

    @pl.when(beam == 0)
    def _():
        turned[:, low, :] = jnp.zeros((2, RIM, flat.shape[2]), F32)
        run_copies([pltpu.make_async_copy(rim, turned.at[:, high, :], in_sem.at[1])])

    @pl.when(beam != 0)
    def _():
        turned[:, high, :] = jnp.zeros((2, RIM, flat.shape[2]), F32)
        run_copies([pltpu.make_async_copy(rim, turned.at[:, low, :], in_sem.at[1])])

    load.wait()
    sends = []

    def send(target, to_rows, to_tile, from_row, count, tile, tile_count):
        sends.append(
            pltpu.make_async_copy(
                turned.at[:, pl.ds(pl.multiple_of(from_row, 8), count), lanes(tile, tile_count)],
                target.at[:, pl.ds(to_rows, count), lanes(to_tile, tile_count)],
                out_sem,
            )
        )

    for step in range(1, 4):
        for k in range(1, GROUP):
            start = jnp.bitwise_xor(mine, k) * sub
            target = outs[3 * (step - 1) + k - 1]
            for position, first, count in spans(plan[step]):
                send(target, 0, position, start, wide, first, count)
            if step == 1:
                for position, first, count in spans(plan[0]):
                    send(target, wide, position, start, RIM, first, count)
                    send(target, wide + RIM, position, start + RIM + sub, RIM, first, count)
    send(own, 0, 0, mine * sub, wide, 0, flat.shape[2] // TILE)
    run_copies(sends)


def pieces(plan, tiles, first, count, sub):
    found = []
    wide = sub + 2 * RIM
    for tile in range(first, first + count):
        to = tile - first
        if tile < 0:
            found.append(["low", 0, wide, 0, 0, to, 1])
        elif tile >= tiles:
            found.append(["high", 0, wide, 0, 0, to, 1])
        else:
            step = next(i for i in range(4) if tile in plan[i])
            at = plan[step].index(tile)
            if step == 0:
                found.append([0, 0, sub, RIM, at, to, 1])
                found.append([1, wide, RIM, 0, at, to, 1])
                found.append([1, wide + RIM, RIM, RIM + sub, at, to, 1])
            else:
                found.append([step, 0, wide, 0, at, to, 1])
    merged = []
    for piece in found:
        for other in merged:
            if (
                other[:4] == piece[:4]
                and other[4] + other[6] == piece[4]
                and other[5] + other[6] == piece[5]
            ):
                other[6] += 1
                break
        else:
            merged.append(list(piece))
    return merged


def raw_copies(plan, tiles, first, count, sub, remote, own, low, high, raw, slot, sem):
    wide = sub + 2 * RIM
    copies = []
    for array, row, rows, to_row, tile, to_tile, width in pieces(plan, tiles, first, count, sub):
        for k in range(GROUP):
            if array in ("low", "high"):
                source = (low if array == "low" else high).at[k]
            elif k == 0:
                continue
            else:
                source = remote[array][k - 1]
            copies.append(
                pltpu.make_async_copy(
                    source.at[:, pl.ds(row, rows), lanes(tile, width)],
                    raw.at[slot(k), :, pl.ds(to_row, rows), lanes(to_tile, width)],
                    sem,
                )
            )
    inner = [t for t in range(first, first + count) if 0 <= t < tiles]
    copies.append(
        pltpu.make_async_copy(
            own.at[:, :, lanes(inner[0], len(inner))],
            raw.at[slot(0), :, pl.ds(0, wide), lanes(inner[0] - first, len(inner))],
            sem,
        )
    )
    return copies


def edge_pack(plan, sub, own, *refs):
    remote = {0: refs[:3], 1: refs[3:6]}
    to_high, to_low, raw, sem, out_sem = refs[6:]
    tiles = own.shape[2] // TILE
    copies = []
    for i, tile in enumerate((tiles - 1, 0)):
        copies += raw_copies(
            plan, tiles, tile, 1, sub, remote, own, None, None, raw.at[i], lambda k: k, sem
        )
    run_copies(copies)
    run_copies(
        [
            pltpu.make_async_copy(raw.at[0], to_high, out_sem),
            pltpu.make_async_copy(raw.at[1], to_low, out_sem),
        ]
    )


def spread(load, store_to, rows, table):
    coarse = table[FINE : FINE + 1, :]
    near, far = coarse == 1.0, coarse == 2.0
    step = 64
    for start in range(0, rows, step):
        size = min(step, rows - start)
        store_to[pl.ds(start, size), :] = jnp.where(
            far, load(start + 16, size), jnp.where(near, load(start + 8, size), load(start, size))
        )


def fine_taps(shifted, start, size, table):
    total = None
    for tap in range(FINE):
        term = table[tap : tap + 1, :] * shifted[pl.ds(start + tap + 4, size), :]
        total = term if total is None else total + term
    return total


def split_into(lhs, at, size, value):
    high = value.astype(BF16)
    low = (value - high.astype(F32)).astype(BF16)
    lhs[pl.ds(at, size), pl.ds(0, TILE)] = high
    lhs[pl.ds(at, size), pl.ds(TILE, TILE)] = low


def turn_factor(base, fine, side, block, start, size):
    base_cos = base[side, 0, pl.ds(block, 1), :]
    base_sin = base[side, 1, pl.ds(block, 1), :]
    fine_cos = fine[side, 0, pl.ds(start, size), :]
    fine_sin = fine[side, 1, pl.ds(start, size), :]
    return base_cos * fine_cos - base_sin * fine_sin, base_sin * fine_cos + base_cos * fine_sin


def merge(plan, steps, runs, sub, has_edges, keep, sc, *refs):
    refs = list(refs)
    own = refs.pop(0)
    low = refs.pop(0) if has_edges else None
    high = refs.pop(0) if has_edges else None
    remote = {}
    for step in steps:
        remote[step] = refs[:3]
        del refs[:3]
    (taps_one, mats_one, lows_one, base_one, fine_one, taps_two, mats_two, base_two, fine_two) = refs[:9]
    del refs[:9]
    if keep:
        refs.pop(0)
    out, raw, flat, shifted, lhs, mixed, parent, done, sems, out_sem = refs
    tiles = own.shape[2] // TILE
    mine, row_base, rows_total = sc[0], sc[2], sc[3]
    wide = sub + 2 * RIM
    half = TILE // 2
    sections = []
    offset = 0
    for index, (first, count) in enumerate(runs):
        copies = raw_copies(
            plan,
            tiles,
            first - 1,
            count + 2,
            sub,
            remote,
            own,
            low,
            high,
            raw.at[:, :, :, pl.ds(offset * TILE, (count + 2) * TILE)],
            lambda k: jnp.bitwise_xor(mine, k),
            sems.at[index],
        )
        for copy in copies:
            copy.start()
        sections.append((offset, copies))
        offset += count + 2
    results = []
    done_at = 0
    for (first, count), (offset, copies) in zip(runs, sections):
        for copy in copies:
            copy.wait()
        blank = jnp.zeros((half - wide, TILE), F32)

        def turn(i, carry):
            for side in range(2):
                for part in range(2):
                    stacked = jnp.concatenate(
                        [
                            raw[2 * side, part, :, lanes(offset + i)],
                            blank,
                            raw[2 * side + 1, part, :, lanes(offset + i)],
                            blank,
                        ],
                        axis=0,
                    )
                    flat[side, part, lanes(i), :] = stacked.T
            return carry

        lax.fori_loop(0, count + 2, turn, 0)
        edges = first == 0 or first + count == tiles

        def parent_block(i, rows):
            for side in range(2):
                for part in range(2):

                    def load(start, size):
                        return flat[
                            side, part, pl.ds(pl.multiple_of(i * TILE + TILE - 2 * HALO + start, 8), size), :
                        ]

                    spread(load, shifted.at[side, part], rows + 24, taps_one[side])
                    for start in range(0, rows, min(rows, half)):
                        size = min(rows, half)
                        split_into(
                            lhs.at[side],
                            part * rows + start,
                            size,
                            fine_taps(shifted.at[side, part], start, size, taps_one[side]),
                        )
                both = pl.ds(0, 2 * rows)
                mixed[side, both, :] = jnp.dot(
                    lhs[side, both, :], mats_one[side], preferred_element_type=F32
                ) + jnp.dot(lhs[side, both, pl.ds(0, TILE)], lows_one[side], preferred_element_type=F32)
            size = min(rows, 32)
            for start in range(0, rows, size):
                sums = [[None, None], [None, None]]
                for side in range(2):
                    cosine, sine = turn_factor(base_one, fine_one, side, first + i, start, size)
                    if edges:
                        row = (
                            lax.broadcasted_iota(jnp.int32, (size, TILE), 0)
                            + row_base
                            + (first + i) * TILE
                            - HALO
                            + start
                        )
                        valid = jnp.logical_and(row >= 0, row < rows_total)
                        cosine = jnp.where(valid, cosine, 0.0)
                        sine = jnp.where(valid, sine, 0.0)
                    for image in range(2):
                        beams = pl.ds(image * TILE, TILE)
                        real = mixed[side, pl.ds(start, size), beams]
                        imag = mixed[side, pl.ds(rows + start, size), beams]
                        terms = (cosine * real - sine * imag, sine * real + cosine * imag)
                        for part in range(2):
                            have = sums[image][part]
                            sums[image][part] = terms[part] if have is None else have + terms[part]
                for image in range(2):
                    for part in range(2):
                        parent[image, part, pl.ds(pl.multiple_of(i * TILE + start, 8), size), :] = sums[
                            image
                        ][part]

        def full_block(i, carry):
            parent_block(i, TILE)
            return carry

        lax.fori_loop(0, count, full_block, 0)
        parent_block(count, 2 * HALO)
        parent[:, :, pl.ds(count * TILE + 2 * HALO, 16), :] = jnp.zeros((2, 2, 16, TILE), F32)

        def final_block(i, carry):
            for image in range(2):
                for part in range(2):

                    def load(start, size):
                        return parent[image, part, pl.ds(pl.multiple_of(i * TILE + start, 8), size), :]

                    spread(load, shifted.at[image, part], TILE + 24, taps_two[image])
                    for start in range(0, TILE, half):
                        split_into(
                            lhs.at[image],
                            part * TILE + start,
                            half,
                            fine_taps(shifted.at[image, part], start, half, taps_two[image]),
                        )
                mixed[image] = jnp.dot(lhs[image], mats_two[image], preferred_element_type=F32)
            size = 32
            for start in range(0, TILE, size):
                sums = [None, None]
                for image in range(2):
                    cosine, sine = turn_factor(base_two, fine_two, image, first + i, start, size)
                    real, imag = (
                        mixed[image, pl.ds(part * TILE + start, size), pl.ds(0, TILE)]
                        + mixed[image, pl.ds(part * TILE + start, size), pl.ds(TILE, TILE)]
                        for part in range(2)
                    )
                    terms = (cosine * real - sine * imag, sine * real + cosine * imag)
                    for part in range(2):
                        sums[part] = terms[part] if sums[part] is None else sums[part] + terms[part]
                for part in range(2):
                    done[part, pl.ds(pl.multiple_of((done_at + i) * TILE + start, 8), size), :] = sums[part]
            return carry

        lax.fori_loop(0, count, final_block, 0)
        result = pltpu.make_async_copy(
            done.at[:, lanes(done_at, count), :], out.at[0, :, lanes(first, count), :], out_sem
        )
        result.start()
        results.append(result)
        done_at += count
    for result in results:
        result.wait()


def window(table, first, count, margin):
    padded = jnp.pad(table, [(0, 0)] * (table.ndim - 1) + [(margin, margin)])
    return lax.dynamic_slice_in_dim(padded, first + margin, count, table.ndim - 1)


def range_table(shifts, taps):
    moved = shifts + SPAN
    fine = moved % TAPS
    spot = lax.broadcasted_iota(jnp.int32, (1, FINE, 1), 1)
    rows = sum(jnp.where(spot - fine[:, None, :] == k, taps[:, k : k + 1, :], 0.0) for k in range(TAPS))
    return jnp.concatenate([rows, (moved // TAPS).astype(F32)[:, None, :]], axis=1)


def beam_matrix(starts, taps, first, height):
    row = lax.broadcasted_iota(jnp.int32, (1, height, 1), 1)
    apart = row - (starts - first)[:, None, :]
    matrix = sum(jnp.where(apart == k, taps[:, k : k + 1, :], 0.0) for k in range(TAPS))
    high = lax.reduce_precision(matrix, 8, 7)
    return high, matrix - high


def turn_tables(rates, offsets, starts, total):
    base = rates[:, None, :] * (starts.astype(F32) / total)[None, :, None] + offsets[:, None, :]
    fine = rates[:, None, :] * (lax.iota(jnp.int32, TILE).astype(F32) / total)[None, :, None]
    return jnp.stack([jnp.cos(base), jnp.sin(base)], 1), jnp.stack([jnp.cos(fine), jnp.sin(fine)], 1)


def body(
    children,
    shift_one,
    rtaps_one,
    bstart_one,
    btaps_one,
    prate_one,
    poff_one,
    shift_two,
    rtaps_two,
    bstart_two,
    btaps_two,
    prate_two,
    poff_two,
):
    rows, blk = children.shape[2], children.shape[3]
    sub = blk // GROUP
    wide = sub + 2 * RIM
    half = TILE // 2
    tiles = rows // TILE
    apers, beams = lax.axis_size("aper"), lax.axis_size("beam")
    total = rows * lax.axis_size("rng")
    assert children.shape[0] == 1 and beams == 2 and apers % GROUP == 0
    assert blk == TILE and rows % (8 * TILE) == 0
    plan = plan_of(tiles)
    mine = lax.axis_index("aper") % GROUP
    beam = lax.axis_index("beam")
    row_base = lax.axis_index("rng") * rows
    sc = jnp.stack([mine, beam, row_base, jnp.int32(total)]).astype(jnp.int32)

    def out(*shape):
        return jax.ShapeDtypeStruct(shape, F32)

    def swap(block, k):
        return lax.ppermute(block, "aper", [(i, i ^ k) for i in range(apers)])

    width = len(plan[0]) * TILE
    *edge, rim, flat = pl.pallas_call(
        functools.partial(first_pack, plan),
        out_shape=[out(2, sub, width)] * 3 + [out(2, RIM, rows), out(2, blk, rows)],
        in_specs=[SMEM, ANY],
        out_specs=[ANY] * 5,
        scratch_shapes=[
            pltpu.VMEM((2, rows, blk), F32),
            pltpu.VMEM((2, blk, rows), F32),
            pltpu.SemaphoreType.DMA((2,)),
            pltpu.SemaphoreType.DMA,
            pltpu.SemaphoreType.DMA,
        ],
        name="first_pack",
    )(sc, children)
    remote = {0: [swap(edge[k - 1], k) for k in range(1, GROUP)]}
    rim = lax.ppermute(rim, "beam", [(0, 1), (1, 0)])
    *packed, own = pl.pallas_call(
        functools.partial(second_pack, plan),
        out_shape=[out(2, wide + 2 * RIM, width)] * 3
        + [out(2, wide, len(plan[2]) * TILE)] * 3
        + [out(2, wide, len(plan[3]) * TILE)] * 3
        + [out(2, wide, rows)],
        in_specs=[SMEM, ANY, ANY],
        out_specs=[ANY] * 10,
        scratch_shapes=[
            pltpu.VMEM((2, blk + 2 * RIM, rows), F32),
            pltpu.SemaphoreType.DMA((2,)),
            pltpu.SemaphoreType.DMA,
        ],
        name="second_pack",
    )(sc, flat, rim)
    for step in range(1, 4):
        remote[step] = [swap(packed[3 * (step - 1) + k - 1], k) for k in range(1, GROUP)]

    to_high, to_low = pl.pallas_call(
        functools.partial(edge_pack, plan, sub),
        out_shape=[out(GROUP, 2, wide, TILE)] * 2,
        in_specs=[ANY] * 7,
        out_specs=[ANY] * 2,
        scratch_shapes=[
            pltpu.VMEM((2, GROUP, 2, wide, TILE), F32),
            pltpu.SemaphoreType.DMA,
            pltpu.SemaphoreType.DMA,
        ],
        name="edge_pack",
    )(own, *remote[0], *remote[1])
    ranks = lax.axis_size("rng")
    low = lax.ppermute(to_high, "rng", [(i, i + 1) for i in range(ranks - 1)])
    high = lax.ppermute(to_low, "rng", [(i + 1, i) for i in range(ranks - 1)])

    block = GROUP * beam + mine
    child_first = sub * block - RIM
    parent_first = 2 * sub * block - PRIM
    final_first = blk * block

    def child_window(table):
        narrow = window(table, child_first, half, half)
        return jnp.concatenate([narrow, narrow], axis=-1)

    def parent_window(table):
        return window(table, parent_first, TILE, TILE)

    def final_window(table):
        return window(table, final_first, TILE, 0)

    taps_one = range_table(child_window(shift_one), child_window(rtaps_one))
    high_one, low_one = beam_matrix(
        parent_window(bstart_one), parent_window(btaps_one), child_first, half
    )

    def paired(matrix):
        none = jnp.zeros_like(matrix)
        return jnp.concatenate(
            [jnp.concatenate([matrix, none], 2), jnp.concatenate([none, matrix], 2)], 1
        ).astype(BF16)

    mats_one = jnp.concatenate([paired(high_one)] * 2, axis=1)
    lows_one = paired(low_one)
    block_rows = row_base + TILE * lax.iota(jnp.int32, tiles + 8)
    base_one, fine_one = turn_tables(
        parent_window(prate_one), parent_window(poff_one), block_rows - HALO, total
    )
    taps_two = range_table(parent_window(shift_two), parent_window(rtaps_two))
    high_two, low_two = beam_matrix(
        final_window(bstart_two), final_window(btaps_two), parent_first, TILE
    )
    mats_two = jnp.concatenate(
        [
            jnp.concatenate([high_two, low_two], 2),
            jnp.concatenate([high_two, jnp.zeros_like(low_two)], 2),
        ],
        1,
    ).astype(BF16)
    base_two, fine_two = turn_tables(
        final_window(prate_two), final_window(poff_two), block_rows, total
    )
    tables = (
        taps_one,
        mats_one,
        lows_one,
        base_one,
        fine_one,
        taps_two,
        mats_two,
        base_two,
        fine_two,
    )

    def merged(name, steps, runs, use_edges, before):
        arrays = [own] + ([low, high] if use_edges else [])
        for step in steps:
            arrays += remote[step]
        longest = max(count for _, count in runs)
        columns = sum(count + 2 for _, count in runs)
        keep = before is not None
        operands = [sc, *arrays, *tables] + ([before] if keep else [])
        return pl.pallas_call(
            functools.partial(merge, plan, steps, runs, sub, use_edges, keep),
            out_shape=out(1, 2, rows, blk),
            in_specs=[SMEM] + [ANY] * len(arrays) + [VMEM] * len(tables) + ([ANY] if keep else []),
            out_specs=ANY,
            input_output_aliases={len(operands) - 1: 0} if keep else {},
            scratch_shapes=[
                pltpu.VMEM((GROUP, 2, wide, columns * TILE), F32),
                pltpu.VMEM((2, 2, (longest + 2) * TILE, TILE), F32),
                pltpu.VMEM((2, 2, TILE + 24, TILE), F32),
                pltpu.VMEM((2, 2 * TILE, 2 * TILE), BF16),
                pltpu.VMEM((2, 2 * TILE, 2 * TILE), F32),
                pltpu.VMEM((2, 2, longest * TILE + 2 * HALO + 16, TILE), F32),
                pltpu.VMEM((2, sum(count for _, count in runs) * TILE, TILE), F32),
                pltpu.SemaphoreType.DMA((len(runs),)),
                pltpu.SemaphoreType.DMA,
            ],
            name=name,
        )(*operands)

    ready_one = plan[1][-1]
    ready_two = plan[2][-1]
    image = merged("merge_b", (0, 1), [(1, ready_one - 1)], False, None)
    image = merged(
        "merge_c",
        (0, 1, 2),
        [(tiles - 1, 1), (0, 1), (ready_one, ready_two - ready_one)],
        True,
        image,
    )
    return merged("merge_d", (0, 1, 2, 3), [(ready_two, tiles - 1 - ready_two)], False, image)


def solution(mesh):
    return jax.shard_map(
        body,
        mesh=mesh,
        in_specs=(P("aper", None, "rng", "beam"),) + (P(),) * 12,
        out_specs=P("aper", None, "rng", "beam"),
        check_vma=False,
    )
```

```python
import functools

import jax
import jax.numpy as jnp
from jax import lax
from jax.experimental import pallas as pl
from jax.experimental.pallas import tpu as pltpu
from jax.sharding import PartitionSpec as P

TAPS = 8
SPAN = 8
GROUP = 4
TILE = 128
RIM = 8
PRIM = 5
HALO = 16
FINE = 2 * TAPS - 1
ANY = pl.BlockSpec(memory_space=pl.ANY)
SMEM = pl.BlockSpec(memory_space=pltpu.SMEM)
VMEM = pl.BlockSpec(memory_space=pltpu.VMEM)
F32 = jnp.float32
BF16 = jnp.bfloat16


def plan_of(tiles):
    quarter = tiles // 4
    half = quarter // 2
    ring = list(range(tiles - half, tiles)) + list(range(tiles - half))
    return [ring[i * quarter : (i + 1) * quarter] for i in range(4)]


def spans(tiles):
    runs = []
    for position, tile in enumerate(tiles):
        if runs and tile == runs[-1][1] + runs[-1][2]:
            runs[-1][2] += 1
        else:
            runs.append([position, tile, 1])
    return runs


def lanes(tile, count=1):
    return pl.ds(tile * TILE, count * TILE)


def fetch(child, rows_in, first, count, sem):
    rows = pl.ds(first * TILE, count * TILE)
    return pltpu.make_async_copy(child.at[0, :, rows, :], rows_in.at[:, rows, :], sem)


def first_pack(plan, sc, child, *refs):
    outs, (rows_in, turned, sem) = refs[:3], refs[3:]
    sub = child.shape[3] // GROUP
    runs = spans(plan[0])
    copies = [fetch(child, rows_in, first, count, sem) for _, first, count in runs]
    for copy in copies:
        copy.start()
    for copy in copies:
        copy.wait()
    for position, tile in enumerate(plan[0]):
        for part in range(2):
            turned[part, :, lanes(position)] = rows_in[part, lanes(tile), :].T
    for k in range(1, GROUP):
        start = pl.multiple_of(jnp.bitwise_xor(sc[0], k) * sub, 8)
        for part in range(2):
            outs[k - 1][part] = turned[part, pl.ds(start, sub), :]


def turn_all(sc, child, rim, turned, rows_in, sems):
    blk = child.shape[3]
    tiles = child.shape[2] // TILE
    step = tiles // 4
    copies = [fetch(child, rows_in, i * step, step, sems.at[i]) for i in range(4)]
    for copy in copies:
        copy.start()
    for i, copy in enumerate(copies):
        copy.wait()

        def turn(j, carry):
            tile = i * step + j
            for part in range(2):
                turned[part, :, lanes(tile)] = rows_in[part, lanes(tile), :].T
            return carry

        lax.fori_loop(0, step, turn, 0, unroll=2)
    side = pl.multiple_of((1 - sc[1]) * (blk - RIM), 8)
    for part in range(2):
        rim[part] = turned[part, pl.ds(side, RIM), :]


def second_pack(plan, sc, turned, rim, *refs):
    outs, (own, full) = refs[:9], refs[9:]
    blk = turned.shape[1]
    sub = blk // GROUP
    wide = sub + 2 * RIM
    upper = sc[1] != 0
    for part in range(2):
        full[part, pl.ds(0, RIM), :] = jnp.where(upper, rim[part], 0.0)
        full[part, pl.ds(RIM, blk), :] = turned[part]
        full[part, pl.ds(RIM + blk, RIM), :] = jnp.where(upper, 0.0, rim[part])
    for part in range(2):
        own[part] = full[part, pl.ds(pl.multiple_of(sc[0] * sub, 8), wide), :]
        for k in range(1, GROUP):
            start = pl.multiple_of(jnp.bitwise_xor(sc[0], k) * sub, 8)
            for step in range(1, 4):
                target = outs[3 * (step - 1) + k - 1]
                for position, first, count in spans(plan[step]):
                    target[part, pl.ds(0, wide), lanes(position, count)] = full[
                        part, pl.ds(start, wide), lanes(first, count)
                    ]
                if step == 1:
                    for position, first, count in spans(plan[0]):
                        for at, row in ((wide, start), (wide + RIM, start + RIM + sub)):
                            target[part, pl.ds(at, RIM), lanes(position, count)] = full[
                                part, pl.ds(pl.multiple_of(row, 8), RIM), lanes(first, count)
                            ]


def raw_beams(plan, sub, own, low, high, remote, k, part, tile):
    wide = sub + 2 * RIM
    tiles = own.shape[2] // TILE
    if tile < 0:
        return low[k, part]
    if tile >= tiles:
        return high[k, part]
    if k == 0:
        return own[part, :, lanes(tile)]
    step = next(i for i in range(4) if tile in plan[i])
    at = plan[step].index(tile)
    if step > 0:
        return remote[step][k - 1][part, pl.ds(0, wide), lanes(at)]
    rims = remote[1][k - 1]
    return jnp.concatenate(
        [
            rims[part, pl.ds(wide, RIM), lanes(at)],
            remote[0][k - 1][part, :, lanes(at)],
            rims[part, pl.ds(wide + RIM, RIM), lanes(at)],
        ],
        axis=0,
    )


def edge_pack(plan, sub, own, *refs):
    remote = {0: refs[:3], 1: refs[3:6]}
    to_high, to_low = refs[6:]
    tiles = own.shape[2] // TILE
    for target, tile in ((to_high, tiles - 1), (to_low, 0)):
        for k in range(GROUP):
            for part in range(2):
                target[k, part] = raw_beams(plan, sub, own, None, None, remote, k, part, tile)


def spread(load, store_to, rows, table):
    coarse = table[FINE : FINE + 1, :]
    near, far = coarse == 1.0, coarse == 2.0
    step = 64
    for start in range(0, rows, step):
        size = min(step, rows - start)
        store_to[pl.ds(start, size), :] = jnp.where(
            far, load(start + 16, size), jnp.where(near, load(start + 8, size), load(start, size))
        )


def fine_taps(shifted, start, size, table):
    total = None
    for tap in range(FINE):
        term = table[tap : tap + 1, :] * shifted[pl.ds(start + tap + 4, size), :]
        total = term if total is None else total + term
    return total


def split_into(lhs, at, size, value):
    high = value.astype(BF16)
    low = (value - high.astype(F32)).astype(BF16)
    lhs[pl.ds(at, size), pl.ds(0, TILE)] = high
    lhs[pl.ds(at, size), pl.ds(TILE, TILE)] = low


def turn_factor(base, fine, side, block, start, size):
    base_cos = base[side, 0, pl.ds(block, 1), :]
    base_sin = base[side, 1, pl.ds(block, 1), :]
    fine_cos = fine[side, 0, pl.ds(start, size), :]
    fine_sin = fine[side, 1, pl.ds(start, size), :]
    return base_cos * fine_cos - base_sin * fine_sin, base_sin * fine_cos + base_cos * fine_sin


def merge(plan, steps, runs, sub, has_edges, keep, sc, *refs):
    refs = list(refs)
    own = refs.pop(0)
    low = refs.pop(0) if has_edges else None
    high = refs.pop(0) if has_edges else None
    remote = {}
    for step in steps:
        remote[step] = refs[:3]
        del refs[:3]
    (taps_one, mats_one, lows_one, base_one, fine_one, taps_two, mats_two, base_two, fine_two) = refs[:9]
    del refs[:9]
    if keep:
        refs.pop(0)
    out, flat, shifted, lhs, mixed, parent, done, out_sem = refs
    tiles = own.shape[2] // TILE
    row_base, rows_total = sc[2], sc[3]
    wide = sub + 2 * RIM
    half = TILE // 2
    blank = jnp.zeros((half - wide, TILE), F32)
    results = []
    done_at = 0
    for first, count in runs:
        for i in range(count + 2):
            for side in range(2):
                for part in range(2):
                    pair = [
                        raw_beams(plan, sub, own, low, high, remote, 2 * side + j, part, first - 1 + i)
                        for j in range(2)
                    ]
                    flat[side, part, lanes(i), :] = jnp.concatenate(
                        [pair[0], blank, pair[1], blank], axis=0
                    ).T
        edges = first == 0 or first + count == tiles

        def parent_block(i, rows):
            for side in range(2):
                for part in range(2):

                    def load(start, size):
                        return flat[
                            side, part, pl.ds(pl.multiple_of(i * TILE + TILE - 2 * HALO + start, 8), size), :
                        ]

                    spread(load, shifted.at[side, part], rows + 24, taps_one[side])
                    for start in range(0, rows, min(rows, half)):
                        size = min(rows, half)
                        split_into(
                            lhs.at[side],
                            part * rows + start,
                            size,
                            fine_taps(shifted.at[side, part], start, size, taps_one[side]),
                        )
                both = pl.ds(0, 2 * rows)
                mixed[side, both, :] = jnp.dot(
                    lhs[side, both, :], mats_one[side], preferred_element_type=F32
                ) + jnp.dot(lhs[side, both, pl.ds(0, TILE)], lows_one[side], preferred_element_type=F32)
            size = min(rows, 32)
            for start in range(0, rows, size):
                sums = [[None, None], [None, None]]
                for side in range(2):
                    cosine, sine = turn_factor(base_one, fine_one, side, first + i, start, size)
                    if edges:
                        row = (
                            lax.broadcasted_iota(jnp.int32, (size, TILE), 0)
                            + row_base
                            + (first + i) * TILE
                            - HALO
                            + start
                        )
                        valid = jnp.logical_and(row >= 0, row < rows_total)
                        cosine = jnp.where(valid, cosine, 0.0)
                        sine = jnp.where(valid, sine, 0.0)
                    for image in range(2):
                        beams = pl.ds(image * TILE, TILE)
                        real = mixed[side, pl.ds(start, size), beams]
                        imag = mixed[side, pl.ds(rows + start, size), beams]
                        terms = (cosine * real - sine * imag, sine * real + cosine * imag)
                        for part in range(2):
                            have = sums[image][part]
                            sums[image][part] = terms[part] if have is None else have + terms[part]
                for image in range(2):
                    for part in range(2):
                        parent[image, part, pl.ds(pl.multiple_of(i * TILE + start, 8), size), :] = sums[
                            image
                        ][part]

        def full_block(i, carry):
            parent_block(i, TILE)
            return carry

        lax.fori_loop(0, count, full_block, 0)
        parent_block(count, 2 * HALO)
        parent[:, :, pl.ds(count * TILE + 2 * HALO, 16), :] = jnp.zeros((2, 2, 16, TILE), F32)

        def final_block(i, carry):
            for image in range(2):
                for part in range(2):

                    def load(start, size):
                        return parent[image, part, pl.ds(pl.multiple_of(i * TILE + start, 8), size), :]

                    spread(load, shifted.at[image, part], TILE + 24, taps_two[image])
                    for start in range(0, TILE, half):
                        split_into(
                            lhs.at[image],
                            part * TILE + start,
                            half,
                            fine_taps(shifted.at[image, part], start, half, taps_two[image]),
                        )
                mixed[image] = jnp.dot(lhs[image], mats_two[image], preferred_element_type=F32)
            size = 32
            for start in range(0, TILE, size):
                sums = [None, None]
                for image in range(2):
                    cosine, sine = turn_factor(base_two, fine_two, image, first + i, start, size)
                    real, imag = (
                        mixed[image, pl.ds(part * TILE + start, size), pl.ds(0, TILE)]
                        + mixed[image, pl.ds(part * TILE + start, size), pl.ds(TILE, TILE)]
                        for part in range(2)
                    )
                    terms = (cosine * real - sine * imag, sine * real + cosine * imag)
                    for part in range(2):
                        sums[part] = terms[part] if sums[part] is None else sums[part] + terms[part]
                for part in range(2):
                    done[part, pl.ds(pl.multiple_of((done_at + i) * TILE + start, 8), size), :] = sums[part]
            return carry

        lax.fori_loop(0, count, final_block, 0)
        result = pltpu.make_async_copy(
            done.at[:, lanes(done_at, count), :], out.at[0, :, lanes(first, count), :], out_sem
        )
        result.start()
        results.append(result)
        done_at += count
    for result in results:
        result.wait()


def make_tables(
    tiles,
    sub,
    sc,
    shift_one,
    rtaps_one,
    bstart_one,
    btaps_one,
    prate_one,
    poff_one,
    shift_two,
    rtaps_two,
    bstart_two,
    btaps_two,
    prate_two,
    poff_two,
    taps_one,
    mats_one,
    lows_one,
    base_one,
    fine_one,
    taps_two,
    mats_two,
    base_two,
    fine_two,
):
    mine, beam, row_base = sc[0], sc[1], sc[2]
    total = sc[3].astype(F32)
    block = GROUP * beam + mine
    half = TILE // 2
    child_first = sub * block - RIM
    parent_first = 2 * sub * block - PRIM
    final_first = 4 * sub * block
    lane = lax.broadcasted_iota(jnp.int32, (TAPS, TILE), 1)

    def windowed(rows, first):
        count = rows.shape[1]
        moved = pltpu.roll(rows, lax.rem(2 * count - first, count), 1)[:, :TILE]
        spot = lane + first
        return jnp.where(jnp.logical_and(spot >= 0, spot < count), moved, jnp.zeros_like(moved))

    def line(table, side, first):
        return windowed(jnp.broadcast_to(table[pl.ds(side, 1), :], (TAPS, table.shape[1])), first)

    def twice(rows):
        return jnp.where(lane < half, rows, pltpu.roll(rows, half, 1))

    def range_table(target, shifts, taps):
        moved = shifts[0:1, :] + SPAN
        spot = lax.broadcasted_iota(jnp.int32, (2 * TAPS, TILE), 0)
        apart = spot - lax.rem(moved, jnp.int32(TAPS))
        total_rows = jnp.zeros((2 * TAPS, TILE), F32)
        for k in range(TAPS):
            total_rows = total_rows + jnp.where(apart == k, taps[k : k + 1, :], 0.0)
        target[...] = jnp.where(spot == FINE, (moved // TAPS).astype(F32), total_rows)

    def beam_matrix(starts, taps, first, height):
        apart = lax.broadcasted_iota(jnp.int32, (height, TILE), 0) - (starts[0:1, :] - first)
        matrix = jnp.zeros((height, TILE), F32)
        for k in range(TAPS):
            matrix = matrix + jnp.where(apart == k, taps[k : k + 1, :], 0.0)
        high = matrix.astype(BF16)
        return high, (matrix - high.astype(F32)).astype(BF16)

    def turn_tables(base, fine, rates, offsets, row_first):
        rate, offset = rates[0:1, :], offsets[0:1, :]
        blocks = base.shape[1]
        start = lax.broadcasted_iota(jnp.int32, (blocks, TILE), 0) * TILE + row_first
        angle = rate * (start.astype(F32) / total) + offset
        base[0] = jnp.cos(angle)
        base[1] = jnp.sin(angle)
        groups = TILE // 8
        coarse = rate * ((lax.broadcasted_iota(jnp.int32, (groups, TILE), 0) * 8).astype(F32) / total)
        small = rate * (lax.broadcasted_iota(jnp.int32, (8, TILE), 0).astype(F32) / total)
        coarse_cos, coarse_sin = jnp.cos(coarse), jnp.sin(coarse)
        small_cos, small_sin = jnp.cos(small), jnp.sin(small)
        for j in range(groups):
            cosine, sine = coarse_cos[j : j + 1, :], coarse_sin[j : j + 1, :]
            fine[0, pl.ds(8 * j, 8), :] = cosine * small_cos - sine * small_sin
            fine[1, pl.ds(8 * j, 8), :] = sine * small_cos + cosine * small_sin

    for slot in range(2):
        side = jnp.bitwise_xor(mine // 2, slot)
        range_table(
            taps_one.at[slot],
            twice(line(shift_one, side, child_first)),
            twice(windowed(rtaps_one[side], child_first)),
        )
        high, low = beam_matrix(
            line(bstart_one, side, parent_first),
            windowed(btaps_one[side], parent_first),
            child_first,
            half,
        )
        for target, value, copies in ((mats_one, high, 2), (lows_one, low, 1)):
            none = jnp.zeros_like(value)
            for i in range(copies):
                target[slot, pl.ds(i * TILE, half), pl.ds(0, TILE)] = value
                target[slot, pl.ds(i * TILE, half), pl.ds(TILE, TILE)] = none
                target[slot, pl.ds(i * TILE + half, half), pl.ds(0, TILE)] = none
                target[slot, pl.ds(i * TILE + half, half), pl.ds(TILE, TILE)] = value
        turn_tables(
            base_one.at[slot],
            fine_one.at[slot],
            line(prate_one, side, parent_first),
            line(poff_one, side, parent_first),
            row_base - HALO,
        )
        side = jnp.bitwise_xor(mine % 2, slot)
        range_table(
            taps_two.at[slot],
            line(shift_two, side, parent_first),
            windowed(rtaps_two[side], parent_first),
        )
        high, low = beam_matrix(
            line(bstart_two, side, final_first),
            windowed(btaps_two[side], final_first),
            parent_first,
            TILE,
        )
        mats_two[slot, pl.ds(0, TILE), pl.ds(0, TILE)] = high
        mats_two[slot, pl.ds(0, TILE), pl.ds(TILE, TILE)] = low
        mats_two[slot, pl.ds(TILE, TILE), pl.ds(0, TILE)] = high
        mats_two[slot, pl.ds(TILE, TILE), pl.ds(TILE, TILE)] = jnp.zeros_like(high)
        turn_tables(
            base_two.at[slot],
            fine_two.at[slot],
            line(prate_two, side, final_first),
            line(poff_two, side, final_first),
            row_base,
        )


def body(
    children,
    shift_one,
    rtaps_one,
    bstart_one,
    btaps_one,
    prate_one,
    poff_one,
    shift_two,
    rtaps_two,
    bstart_two,
    btaps_two,
    prate_two,
    poff_two,
):
    rows, blk = children.shape[2], children.shape[3]
    sub = blk // GROUP
    wide = sub + 2 * RIM
    half = TILE // 2
    tiles = rows // TILE
    apers, beams = lax.axis_size("aper"), lax.axis_size("beam")
    total = rows * lax.axis_size("rng")
    assert children.shape[0] == 1 and beams == 2 and apers % GROUP == 0
    assert blk == TILE and rows % (8 * TILE) == 0
    plan = plan_of(tiles)
    mine = lax.axis_index("aper") % GROUP
    beam = lax.axis_index("beam")
    row_base = lax.axis_index("rng") * rows
    sc = jnp.stack([mine, beam, row_base, jnp.int32(total)]).astype(jnp.int32)

    def out(*shape):
        return jax.ShapeDtypeStruct(shape, F32)

    def swap(block, k):
        return lax.ppermute(block, "aper", [(i, i ^ k) for i in range(apers)])

    widths = [len(part) * TILE for part in plan]
    edge = pl.pallas_call(
        functools.partial(first_pack, plan),
        out_shape=[out(2, sub, widths[0])] * 3,
        in_specs=[SMEM, ANY],
        out_specs=[VMEM] * 3,
        scratch_shapes=[
            pltpu.VMEM((2, rows, blk), F32),
            pltpu.VMEM((2, blk, widths[0]), F32),
            pltpu.SemaphoreType.DMA,
        ],
        name="first_pack",
    )(sc, children)
    remote = {0: [swap(edge[k - 1], k) for k in range(1, GROUP)]}
    rim, turned = pl.pallas_call(
        turn_all,
        out_shape=[out(2, RIM, rows), out(2, blk, rows)],
        in_specs=[SMEM, ANY],
        out_specs=[VMEM] * 2,
        scratch_shapes=[pltpu.VMEM((2, rows, blk), F32), pltpu.SemaphoreType.DMA((4,))],
        name="turn_all",
    )(sc, children)
    rim = lax.ppermute(rim, "beam", [(0, 1), (1, 0)])
    *packed, own = pl.pallas_call(
        functools.partial(second_pack, plan),
        out_shape=[out(2, wide + 2 * RIM, widths[1])] * 3
        + [out(2, wide, widths[2])] * 3
        + [out(2, wide, widths[3])] * 3
        + [out(2, wide, rows)],
        in_specs=[SMEM, VMEM, VMEM],
        out_specs=[VMEM] * 10,
        scratch_shapes=[pltpu.VMEM((2, blk + 2 * RIM, rows), F32)],
        name="second_pack",
    )(sc, turned, rim)
    for step in range(1, 4):
        remote[step] = [swap(packed[3 * (step - 1) + k - 1], k) for k in range(1, GROUP)]

    to_high, to_low = pl.pallas_call(
        functools.partial(edge_pack, plan, sub),
        out_shape=[out(GROUP, 2, wide, TILE)] * 2,
        in_specs=[VMEM] * 7,
        out_specs=[VMEM] * 2,
        name="edge_pack",
    )(own, *remote[0], *remote[1])
    ranks = lax.axis_size("rng")
    low = lax.ppermute(to_high, "rng", [(i, i + 1) for i in range(ranks - 1)])
    high = lax.ppermute(to_low, "rng", [(i + 1, i) for i in range(ranks - 1)])

    def brief(*shape):
        return jax.ShapeDtypeStruct(shape, BF16)

    blocks = tiles + 8
    given = (
        shift_one,
        rtaps_one,
        bstart_one,
        btaps_one,
        prate_one,
        poff_one,
        shift_two,
        rtaps_two,
        bstart_two,
        btaps_two,
        prate_two,
        poff_two,
    )
    tables = pl.pallas_call(
        functools.partial(make_tables, tiles, sub),
        out_shape=[
            out(2, 2 * TAPS, TILE),
            brief(2, 2 * TILE, 2 * TILE),
            brief(2, TILE, 2 * TILE),
            out(2, 2, blocks, TILE),
            out(2, 2, TILE, TILE),
            out(2, 2 * TAPS, TILE),
            brief(2, 2 * TILE, 2 * TILE),
            out(2, 2, blocks, TILE),
            out(2, 2, TILE, TILE),
        ],
        in_specs=[SMEM] + [VMEM] * len(given),
        out_specs=[VMEM] * 9,
        name="make_tables",
    )(sc, *given)

    def merged(name, steps, runs, use_edges, before):
        arrays = [own] + ([low, high] if use_edges else [])
        for step in steps:
            arrays += remote[step]
        longest = max(count for _, count in runs)
        keep = before is not None
        operands = [sc, *arrays, *tables] + ([before] if keep else [])
        return pl.pallas_call(
            functools.partial(merge, plan, steps, runs, sub, use_edges, keep),
            out_shape=out(1, 2, rows, blk),
            in_specs=[SMEM] + [VMEM] * (len(arrays) + len(tables)) + ([ANY] if keep else []),
            out_specs=ANY,
            input_output_aliases={len(operands) - 1: 0} if keep else {},
            scratch_shapes=[
                pltpu.VMEM((2, 2, (longest + 2) * TILE, TILE), F32),
                pltpu.VMEM((2, 2, TILE + 24, TILE), F32),
                pltpu.VMEM((2, 2 * TILE, 2 * TILE), BF16),
                pltpu.VMEM((2, 2 * TILE, 2 * TILE), F32),
                pltpu.VMEM((2, 2, longest * TILE + 2 * HALO + 16, TILE), F32),
                pltpu.VMEM((2, sum(count for _, count in runs) * TILE, TILE), F32),
                pltpu.SemaphoreType.DMA,
            ],
            name=name,
        )(*operands)

    ready_one = plan[1][-1]
    ready_two = plan[2][-1]
    image = merged("merge_b", (0, 1), [(1, ready_one - 1)], False, None)
    image = merged(
        "merge_c",
        (0, 1, 2),
        [(tiles - 1, 1), (0, 1), (ready_one, ready_two - ready_one)],
        True,
        image,
    )
    return merged("merge_d", (0, 1, 2, 3), [(ready_two, tiles - 1 - ready_two)], False, image)


def solution(mesh):
    return jax.shard_map(
        body,
        mesh=mesh,
        in_specs=(P("aper", None, "rng", "beam"),) + (P(),) * 12,
        out_specs=P("aper", None, "rng", "beam"),
        check_vma=False,
    )
```

```python
import functools

import jax
import jax.numpy as jnp
from jax import lax
from jax.experimental import pallas as pl
from jax.experimental.pallas import tpu as pltpu
from jax.sharding import PartitionSpec as P


TAPS = 8
SPAN = 8
GROUP = 4
TILE = 128
RIM = 8
PRIM = 5
HALO = 16
FINE = 2 * TAPS - 1
ANY = pl.BlockSpec(memory_space=pl.ANY)
HBM = pl.BlockSpec(memory_space=pltpu.HBM)
SMEM = pl.BlockSpec(memory_space=pltpu.SMEM)
VMEM = pl.BlockSpec(memory_space=pltpu.VMEM)
F32 = jnp.float32
BF16 = jnp.bfloat16
PARAMS = pltpu.CompilerParams(vmem_limit_bytes=24 << 20)


def plan_of(tiles):
    quarter = tiles // 4
    half = quarter // 2
    ring = list(range(tiles - half, tiles)) + list(range(tiles - half))
    return [ring[i * quarter : (i + 1) * quarter] for i in range(4)]


def spans(tiles):
    runs = []
    for position, tile in enumerate(tiles):
        if runs and tile == runs[-1][1] + runs[-1][2]:
            runs[-1][2] += 1
        else:
            runs.append([position, tile, 1])
    return runs


def lanes(tile, count=1):
    return pl.ds(tile * TILE, count * TILE)


def fetch(child, rows_in, first, count, sem):
    rows = pl.ds(first * TILE, count * TILE)
    return pltpu.make_async_copy(child.at[0, :, rows, :], rows_in.at[:, rows, :], sem)


def first_pack(plan, sc, child, *refs):
    outs, (rows_in, turned, sem) = refs[:3], refs[3:]
    sub = child.shape[3] // GROUP
    runs = spans(plan[0])
    copies = [fetch(child, rows_in, first, count, sem) for _, first, count in runs]
    for copy in copies:
        copy.start()
    for copy in copies:
        copy.wait()
    for position, tile in enumerate(plan[0]):
        for part in range(2):
            turned[part, :, lanes(position)] = rows_in[part, lanes(tile), :].T
    for k in range(1, GROUP):
        start = pl.multiple_of(jnp.bitwise_xor(sc[0], k) * sub, 8)
        for part in range(2):
            outs[k - 1][part] = turned[part, pl.ds(start, sub), :]


def turn_all(sc, child, after, rim, turned, rows_in, sems):
    del after
    blk = child.shape[3]
    tiles = child.shape[2] // TILE
    step = tiles // 4
    copies = [fetch(child, rows_in, i * step, step, sems.at[i]) for i in range(4)]
    for copy in copies:
        copy.start()
    for i, copy in enumerate(copies):
        copy.wait()

        def turn(j, carry):
            tile = i * step + j
            for part in range(2):
                turned[part, :, lanes(tile)] = rows_in[part, lanes(tile), :].T
            return carry

        lax.fori_loop(0, step, turn, 0, unroll=2)
    side = pl.multiple_of((1 - sc[1]) * (blk - RIM), 8)
    for part in range(2):
        rim[part] = turned[part, pl.ds(side, RIM), :]


def second_pack(plan, sc, turned, rim, *refs):
    outs, (own, full) = refs[:9], refs[9:]
    blk = turned.shape[1]
    sub = blk // GROUP
    wide = sub + 2 * RIM
    upper = sc[1] != 0
    for part in range(2):
        full[part, pl.ds(0, RIM), :] = jnp.where(upper, rim[part], 0.0)
        full[part, pl.ds(RIM, blk), :] = turned[part]
        full[part, pl.ds(RIM + blk, RIM), :] = jnp.where(upper, 0.0, rim[part])
    for part in range(2):
        own[part] = full[part, pl.ds(pl.multiple_of(sc[0] * sub, 8), wide), :]
        for k in range(1, GROUP):
            start = pl.multiple_of(jnp.bitwise_xor(sc[0], k) * sub, 8)
            for step in range(1, 4):
                target = outs[3 * (step - 1) + k - 1]
                for position, first, count in spans(plan[step]):
                    target[part, pl.ds(0, wide), lanes(position, count)] = full[
                        part, pl.ds(start, wide), lanes(first, count)
                    ]
                if step == 1:
                    for position, first, count in spans(plan[0]):
                        for at, row in ((wide, start), (wide + RIM, start + RIM + sub)):
                            target[part, pl.ds(at, RIM), lanes(position, count)] = full[
                                part, pl.ds(pl.multiple_of(row, 8), RIM), lanes(first, count)
                            ]


def raw_beams(plan, sub, own, low, high, remote, k, part, tile):
    wide = sub + 2 * RIM
    tiles = own.shape[2] // TILE
    if tile < 0:
        return low[k, part]
    if tile >= tiles:
        return high[k, part]
    if k == 0:
        return own[part, :, lanes(tile)]
    step = next(i for i in range(4) if tile in plan[i])
    at = plan[step].index(tile)
    if step > 0:
        return remote[step][k - 1][part, pl.ds(0, wide), lanes(at)]
    rims = remote[1][k - 1]
    return jnp.concatenate(
        [
            rims[part, pl.ds(wide, RIM), lanes(at)],
            remote[0][k - 1][part, :, lanes(at)],
            rims[part, pl.ds(wide + RIM, RIM), lanes(at)],
        ],
        axis=0,
    )


def edge_pack(plan, sub, own, *refs):
    remote = {0: refs[:3], 1: refs[3:6]}
    to_high, to_low = refs[6:]
    tiles = own.shape[2] // TILE
    for target, tile in ((to_high, tiles - 1), (to_low, 0)):
        for k in range(GROUP):
            for part in range(2):
                target[k, part] = raw_beams(plan, sub, own, None, None, remote, k, part, tile)


def spread(load, store_to, rows, table):
    coarse = table[FINE : FINE + 1, :]
    near, far = coarse == 1.0, coarse == 2.0
    step = 64
    for start in range(0, rows, step):
        size = min(step, rows - start)
        store_to[pl.ds(start, size), :] = jnp.where(
            far, load(start + 16, size), jnp.where(near, load(start + 8, size), load(start, size))
        )


def fine_taps(shifted, start, size, table):
    total = None
    for tap in range(FINE):
        term = table[tap : tap + 1, :] * shifted[pl.ds(start + tap + 4, size), :]
        total = term if total is None else total + term
    return total


def split_into(lhs, at, size, value):
    high = value.astype(BF16)
    low = (value - high.astype(F32)).astype(BF16)
    lhs[pl.ds(at, size), pl.ds(0, TILE)] = high
    lhs[pl.ds(at, size), pl.ds(TILE, TILE)] = low


def turn_factor(base, fine, side, block, start, size):
    base_cos = base[side, 0, pl.ds(block, 1), :]
    base_sin = base[side, 1, pl.ds(block, 1), :]
    fine_cos = fine[side, 0, pl.ds(start, size), :]
    fine_sin = fine[side, 1, pl.ds(start, size), :]
    return base_cos * fine_cos - base_sin * fine_sin, base_sin * fine_cos + base_cos * fine_sin


def merge(plan, steps, runs, sub, has_edges, keep, sc, *refs):
    refs = list(refs)
    own = refs.pop(0)
    low = refs.pop(0) if has_edges else None
    high = refs.pop(0) if has_edges else None
    remote = {}
    for step in steps:
        remote[step] = refs[:3]
        del refs[:3]
    (taps_one, mats_one, lows_one, base_one, fine_one, taps_two, mats_two, base_two, fine_two) = refs[:9]
    del refs[:9]
    if keep:
        refs.pop(0)
    out, flat, shifted, lhs, mixed, parent, done, out_sem = refs
    tiles = own.shape[2] // TILE
    row_base, rows_total = sc[2], sc[3]
    wide = sub + 2 * RIM
    half = TILE // 2
    blank = jnp.zeros((half - wide, TILE), F32)
    results = []
    done_at = 0
    for first, count in runs:
        for i in range(count + 2):
            for side in range(2):
                for part in range(2):
                    pair = [
                        raw_beams(plan, sub, own, low, high, remote, 2 * side + j, part, first - 1 + i)
                        for j in range(2)
                    ]
                    flat[side, part, lanes(i), :] = jnp.concatenate(
                        [pair[0], blank, pair[1], blank], axis=0
                    ).T
        edges = first == 0 or first + count == tiles

        def parent_block(i, rows):
            for side in range(2):
                for part in range(2):

                    def load(start, size):
                        return flat[
                            side, part, pl.ds(pl.multiple_of(i * TILE + TILE - 2 * HALO + start, 8), size), :
                        ]

                    spread(load, shifted.at[side, part], rows + 24, taps_one[side])
                    for start in range(0, rows, min(rows, half)):
                        size = min(rows, half)
                        split_into(
                            lhs.at[side],
                            part * rows + start,
                            size,
                            fine_taps(shifted.at[side, part], start, size, taps_one[side]),
                        )
                both = pl.ds(0, 2 * rows)
                mixed[side, both, :] = jnp.dot(
                    lhs[side, both, :], mats_one[side], preferred_element_type=F32
                ) + jnp.dot(lhs[side, both, pl.ds(0, TILE)], lows_one[side], preferred_element_type=F32)
            size = min(rows, 32)
            for start in range(0, rows, size):
                sums = [[None, None], [None, None]]
                for side in range(2):
                    cosine, sine = turn_factor(base_one, fine_one, side, first + i, start, size)
                    if edges:
                        row = (
                            lax.broadcasted_iota(jnp.int32, (size, TILE), 0)
                            + row_base
                            + (first + i) * TILE
                            - HALO
                            + start
                        )
                        valid = jnp.logical_and(row >= 0, row < rows_total)
                        cosine = jnp.where(valid, cosine, 0.0)
                        sine = jnp.where(valid, sine, 0.0)
                    for image in range(2):
                        beams = pl.ds(image * TILE, TILE)
                        real = mixed[side, pl.ds(start, size), beams]
                        imag = mixed[side, pl.ds(rows + start, size), beams]
                        terms = (cosine * real - sine * imag, sine * real + cosine * imag)
                        for part in range(2):
                            have = sums[image][part]
                            sums[image][part] = terms[part] if have is None else have + terms[part]
                for image in range(2):
                    for part in range(2):
                        parent[image, part, pl.ds(pl.multiple_of(i * TILE + start, 8), size), :] = sums[
                            image
                        ][part]

        def full_block(i, carry):
            parent_block(i, TILE)
            return carry

        lax.fori_loop(0, count, full_block, 0)
        parent_block(count, 2 * HALO)
        parent[:, :, pl.ds(count * TILE + 2 * HALO, 16), :] = jnp.zeros((2, 2, 16, TILE), F32)

        def final_block(i, carry):
            for image in range(2):
                for part in range(2):

                    def load(start, size):
                        return parent[image, part, pl.ds(pl.multiple_of(i * TILE + start, 8), size), :]

                    spread(load, shifted.at[image, part], TILE + 24, taps_two[image])
                    for start in range(0, TILE, half):
                        split_into(
                            lhs.at[image],
                            part * TILE + start,
                            half,
                            fine_taps(shifted.at[image, part], start, half, taps_two[image]),
                        )
                mixed[image] = jnp.dot(lhs[image], mats_two[image], preferred_element_type=F32)
            size = 32
            for start in range(0, TILE, size):
                sums = [None, None]
                for image in range(2):
                    cosine, sine = turn_factor(base_two, fine_two, image, first + i, start, size)
                    real, imag = (
                        mixed[image, pl.ds(part * TILE + start, size), pl.ds(0, TILE)]
                        + mixed[image, pl.ds(part * TILE + start, size), pl.ds(TILE, TILE)]
                        for part in range(2)
                    )
                    terms = (cosine * real - sine * imag, sine * real + cosine * imag)
                    for part in range(2):
                        sums[part] = terms[part] if sums[part] is None else sums[part] + terms[part]
                for part in range(2):
                    done[part, pl.ds(pl.multiple_of((done_at + i) * TILE + start, 8), size), :] = sums[part]
            return carry

        lax.fori_loop(0, count, final_block, 0)
        result = pltpu.make_async_copy(
            done.at[:, lanes(done_at, count), :], out.at[0, :, lanes(first, count), :], out_sem
        )
        result.start()
        results.append(result)
        done_at += count
    for result in results:
        result.wait()


def make_tables(
    sub,
    sc,
    shift_one,
    rtaps_one,
    bstart_one,
    btaps_one,
    prate_one,
    poff_one,
    shift_two,
    rtaps_two,
    bstart_two,
    btaps_two,
    prate_two,
    poff_two,
    taps_one,
    mats_one,
    lows_one,
    base_one,
    fine_one,
    taps_two,
    mats_two,
    base_two,
    fine_two,
):
    mine, beam, row_base = sc[0], sc[1], sc[2]
    total = sc[3].astype(F32)
    block = GROUP * beam + mine
    half = TILE // 2
    child_first = sub * block - RIM
    parent_first = 2 * sub * block - PRIM
    final_first = 4 * sub * block
    lane = lax.broadcasted_iota(jnp.int32, (TAPS, TILE), 1)

    def windowed(rows, first):
        count = rows.shape[1]
        moved = pltpu.roll(rows, lax.rem(2 * count - first, count), 1)[:, :TILE]
        spot = lane + first
        return jnp.where(jnp.logical_and(spot >= 0, spot < count), moved, jnp.zeros_like(moved))

    def line(table, side, first):
        return windowed(jnp.broadcast_to(table[pl.ds(side, 1), :], (TAPS, table.shape[1])), first)

    def twice(rows):
        return jnp.where(lane < half, rows, pltpu.roll(rows, half, 1))

    def range_table(target, shifts, taps):
        moved = shifts[0:1, :] + SPAN
        spot = lax.broadcasted_iota(jnp.int32, (2 * TAPS, TILE), 0)
        apart = spot - lax.rem(moved, jnp.int32(TAPS))
        total_rows = jnp.zeros((2 * TAPS, TILE), F32)
        for k in range(TAPS):
            total_rows = total_rows + jnp.where(apart == k, taps[k : k + 1, :], 0.0)
        target[...] = jnp.where(spot == FINE, (moved // TAPS).astype(F32), total_rows)

    def beam_matrix(starts, taps, first, height):
        apart = lax.broadcasted_iota(jnp.int32, (height, TILE), 0) - (starts[0:1, :] - first)
        matrix = jnp.zeros((height, TILE), F32)
        for k in range(TAPS):
            matrix = matrix + jnp.where(apart == k, taps[k : k + 1, :], 0.0)
        high = matrix.astype(BF16)
        return high, (matrix - high.astype(F32)).astype(BF16)

    def turn_tables(base, fine, rates, offsets, row_first):
        rate, offset = rates[0:1, :], offsets[0:1, :]
        blocks = base.shape[1]
        start = lax.broadcasted_iota(jnp.int32, (blocks, TILE), 0) * TILE + row_first
        angle = rate * (start.astype(F32) / total) + offset
        base[0] = jnp.cos(angle)
        base[1] = jnp.sin(angle)
        groups = TILE // 8
        coarse = rate * ((lax.broadcasted_iota(jnp.int32, (groups, TILE), 0) * 8).astype(F32) / total)
        small = rate * (lax.broadcasted_iota(jnp.int32, (8, TILE), 0).astype(F32) / total)
        coarse_cos, coarse_sin = jnp.cos(coarse), jnp.sin(coarse)
        small_cos, small_sin = jnp.cos(small), jnp.sin(small)
        for j in range(groups):
            cosine, sine = coarse_cos[j : j + 1, :], coarse_sin[j : j + 1, :]
            fine[0, pl.ds(8 * j, 8), :] = cosine * small_cos - sine * small_sin
            fine[1, pl.ds(8 * j, 8), :] = sine * small_cos + cosine * small_sin

    for slot in range(2):
        side = jnp.bitwise_xor(mine // 2, slot)
        range_table(
            taps_one.at[slot],
            twice(line(shift_one, side, child_first)),
            twice(windowed(rtaps_one[side], child_first)),
        )
        high, low = beam_matrix(
            line(bstart_one, side, parent_first),
            windowed(btaps_one[side], parent_first),
            child_first,
            half,
        )
        for target, value, copies in ((mats_one, high, 2), (lows_one, low, 1)):
            none = jnp.zeros_like(value)
            for i in range(copies):
                target[slot, pl.ds(i * TILE, half), pl.ds(0, TILE)] = value
                target[slot, pl.ds(i * TILE, half), pl.ds(TILE, TILE)] = none
                target[slot, pl.ds(i * TILE + half, half), pl.ds(0, TILE)] = none
                target[slot, pl.ds(i * TILE + half, half), pl.ds(TILE, TILE)] = value
        turn_tables(
            base_one.at[slot],
            fine_one.at[slot],
            line(prate_one, side, parent_first),
            line(poff_one, side, parent_first),
            row_base - HALO,
        )
        side = jnp.bitwise_xor(mine % 2, slot)
        range_table(
            taps_two.at[slot],
            line(shift_two, side, parent_first),
            windowed(rtaps_two[side], parent_first),
        )
        high, low = beam_matrix(
            line(bstart_two, side, final_first),
            windowed(btaps_two[side], final_first),
            parent_first,
            TILE,
        )
        mats_two[slot, pl.ds(0, TILE), pl.ds(0, TILE)] = high
        mats_two[slot, pl.ds(0, TILE), pl.ds(TILE, TILE)] = low
        mats_two[slot, pl.ds(TILE, TILE), pl.ds(0, TILE)] = high
        mats_two[slot, pl.ds(TILE, TILE), pl.ds(TILE, TILE)] = jnp.zeros_like(high)
        turn_tables(
            base_two.at[slot],
            fine_two.at[slot],
            line(prate_two, side, final_first),
            line(poff_two, side, final_first),
            row_base,
        )


def body(
    children,
    shift_one,
    rtaps_one,
    bstart_one,
    btaps_one,
    prate_one,
    poff_one,
    shift_two,
    rtaps_two,
    bstart_two,
    btaps_two,
    prate_two,
    poff_two,
):
    rows, blk = children.shape[2], children.shape[3]
    sub = blk // GROUP
    wide = sub + 2 * RIM
    tiles = rows // TILE
    apers, beams = lax.axis_size("aper"), lax.axis_size("beam")
    total = rows * lax.axis_size("rng")
    assert children.shape[0] == 1 and beams == 2 and apers % GROUP == 0
    assert blk == TILE and rows % (8 * TILE) == 0
    plan = plan_of(tiles)
    mine = lax.axis_index("aper") % GROUP
    beam = lax.axis_index("beam")
    row_base = lax.axis_index("rng") * rows
    sc = jnp.stack([mine, beam, row_base, jnp.int32(total)]).astype(jnp.int32)

    def out(*shape):
        return pltpu.VMEM(shape, F32)

    def near(arrays):
        return [pltpu.with_memory_space_constraint(array, pltpu.VMEM) for array in arrays]

    def call(kernel, *operands, **settings):
        return pl.pallas_call(kernel, compiler_params=PARAMS, **settings)(*operands)

    def swap(block, k):
        return lax.ppermute(block, "aper", [(i, i ^ k) for i in range(apers)])

    children = pltpu.with_memory_space_constraint(children, pltpu.HBM)
    widths = [len(part) * TILE for part in plan]
    edge = call(
        functools.partial(first_pack, plan),
        sc, children,
        out_shape=[out(2, sub, widths[0])] * 3,
        in_specs=[SMEM, HBM],
        out_specs=[VMEM] * 3,
        scratch_shapes=[
            pltpu.VMEM((2, rows, blk), F32),
            pltpu.VMEM((2, blk, widths[0]), F32),
            pltpu.SemaphoreType.DMA,
        ],
    )
    remote = {0: [swap(edge[k - 1], k) for k in range(1, GROUP)]}
    rim, turned = call(
        turn_all,
        sc, children, edge[0],
        out_shape=[out(2, RIM, rows), out(2, blk, rows)],
        in_specs=[SMEM, HBM, ANY],
        out_specs=[VMEM] * 2,
        scratch_shapes=[pltpu.VMEM((2, rows, blk), F32), pltpu.SemaphoreType.DMA((4,))],
    )
    rim = lax.ppermute(rim, "beam", [(0, 1), (1, 0)])
    *packed, own = call(
        functools.partial(second_pack, plan),
        sc, *near([turned, rim]),
        out_shape=[out(2, wide + 2 * RIM, widths[1])] * 3
        + [out(2, wide, widths[2])] * 3
        + [out(2, wide, widths[3])] * 3
        + [out(2, wide, rows)],
        in_specs=[SMEM, VMEM, VMEM],
        out_specs=[VMEM] * 10,
        scratch_shapes=[pltpu.VMEM((2, blk + 2 * RIM, rows), F32)],
    )
    for step in range(1, 4):
        remote[step] = [swap(packed[3 * (step - 1) + k - 1], k) for k in range(1, GROUP)]

    to_high, to_low = call(
        functools.partial(edge_pack, plan, sub),
        *near([own, *remote[0], *remote[1]]),
        out_shape=[out(GROUP, 2, wide, TILE)] * 2,
        in_specs=[VMEM] * 7,
        out_specs=[VMEM] * 2,
    )
    ranks = lax.axis_size("rng")
    low = lax.ppermute(to_high, "rng", [(i, i + 1) for i in range(ranks - 1)])
    high = lax.ppermute(to_low, "rng", [(i + 1, i) for i in range(ranks - 1)])

    def brief(*shape):
        return pltpu.VMEM(shape, BF16)

    blocks = tiles + 8
    given = (
        shift_one,
        rtaps_one,
        bstart_one,
        btaps_one,
        prate_one,
        poff_one,
        shift_two,
        rtaps_two,
        bstart_two,
        btaps_two,
        prate_two,
        poff_two,
    )
    tables = call(
        functools.partial(make_tables, sub),
        sc, *given,
        out_shape=[
            out(2, 2 * TAPS, TILE),
            brief(2, 2 * TILE, 2 * TILE),
            brief(2, TILE, 2 * TILE),
            out(2, 2, blocks, TILE),
            out(2, 2, TILE, TILE),
            out(2, 2 * TAPS, TILE),
            brief(2, 2 * TILE, 2 * TILE),
            out(2, 2, blocks, TILE),
            out(2, 2, TILE, TILE),
        ],
        in_specs=[SMEM] + [VMEM] * len(given),
        out_specs=[VMEM] * 9,
    )

    def merged(steps, runs, use_edges, before):
        arrays = [own] + ([low, high] if use_edges else [])
        for step in steps:
            arrays += remote[step]
        longest = max(count for _, count in runs)
        keep = before is not None
        operands = [sc, *near([*arrays, *tables])] + ([before] if keep else [])
        return call(
            functools.partial(merge, plan, steps, runs, sub, use_edges, keep),
            *operands,
            out_shape=jax.ShapeDtypeStruct((1, 2, rows, blk), F32),
            in_specs=[SMEM] + [VMEM] * (len(arrays) + len(tables)) + ([ANY] if keep else []),
            out_specs=ANY,
            input_output_aliases={len(operands) - 1: 0} if keep else {},
            scratch_shapes=[
                pltpu.VMEM((2, 2, (longest + 2) * TILE, TILE), F32),
                pltpu.VMEM((2, 2, TILE + 24, TILE), F32),
                pltpu.VMEM((2, 2 * TILE, 2 * TILE), BF16),
                pltpu.VMEM((2, 2 * TILE, 2 * TILE), F32),
                pltpu.VMEM((2, 2, longest * TILE + 2 * HALO + 16, TILE), F32),
                pltpu.VMEM((2, sum(count for _, count in runs) * TILE, TILE), F32),
                pltpu.SemaphoreType.DMA,
            ],
        )

    ready_one = plan[1][-1]
    ready_two = plan[2][-1]
    image = merged((0, 1), [(1, ready_one - 1)], False, None)
    image = merged(
        (0, 1, 2), [(tiles - 1, 1), (0, 1), (ready_one, ready_two - ready_one)], True, image
    )
    return merged((0, 1, 2, 3), [(ready_two, tiles - 1 - ready_two)], False, image)


def solution(mesh):
    return jax.shard_map(
        body,
        mesh=mesh,
        in_specs=(P("aper", None, "rng", "beam"),) + (P(),) * 12,
        out_specs=P("aper", None, "rng", "beam"),
        check_vma=False,
    )
```

```python
import functools

import jax
import jax.numpy as jnp
from jax import lax
from jax.experimental import pallas as pl
from jax.experimental.pallas import tpu as pltpu
from jax.sharding import PartitionSpec as P


TAPS = 8
SPAN = 8
GROUP = 4
TILE = 128
RIM = 8
PRIM = 5
HALO = 16
COARSE = 4
FINE = TAPS + COARSE - 1
ANY = pl.BlockSpec(memory_space=pl.ANY)
HBM = pl.BlockSpec(memory_space=pltpu.HBM)
SMEM = pl.BlockSpec(memory_space=pltpu.SMEM)
VMEM = pl.BlockSpec(memory_space=pltpu.VMEM)
F32 = jnp.float32
BF16 = jnp.bfloat16
PARAMS = pltpu.CompilerParams(vmem_limit_bytes=24 << 20)


def plan_of(tiles):
    quarter = tiles // 4
    half = quarter // 2
    ring = list(range(tiles - half, tiles)) + list(range(tiles - half))
    return [ring[i * quarter : (i + 1) * quarter] for i in range(4)]


def spans(tiles):
    runs = []
    for position, tile in enumerate(tiles):
        if runs and tile == runs[-1][1] + runs[-1][2]:
            runs[-1][2] += 1
        else:
            runs.append([position, tile, 1])
    return runs


def lanes(tile, count=1):
    return pl.ds(tile * TILE, count * TILE)


def fetch(child, rows_in, first, count, sem):
    rows = pl.ds(first * TILE, count * TILE)
    return pltpu.make_async_copy(child.at[0, :, rows, :], rows_in.at[:, rows, :], sem)


def first_pack(plan, sc, child, *refs):
    outs, (rim, turned, rows_in, sems) = refs[:3], refs[3:]
    blk = child.shape[3]
    sub = blk // GROUP
    parts = [spans(part) for part in plan]
    copies = [
        [fetch(child, rows_in, first, count, sems.at[i]) for _, first, count in part]
        for i, part in enumerate(parts)
    ]
    for part in copies:
        for copy in part:
            copy.start()
    for i, part in enumerate(copies):
        for copy in part:
            copy.wait()
        for tile in plan[i]:
            for part in range(2):
                turned[part, :, lanes(tile)] = rows_in[part, lanes(tile), :].T
        if i == 0:
            for k in range(1, GROUP):
                start = pl.multiple_of(jnp.bitwise_xor(sc[0], k) * sub, 8)
                for position, first, count in parts[0]:
                    outs[k - 1][:, :, lanes(position, count)] = turned[
                        :, pl.ds(start, sub), lanes(first, count)
                    ]
    side = pl.multiple_of((1 - sc[1]) * (blk - RIM), 8)
    rim[...] = turned[:, pl.ds(side, RIM), :]


def second_pack(plan, sc, turned, rim, *refs):
    outs, (own, full) = refs[:9], refs[9:]
    blk = turned.shape[1]
    sub = blk // GROUP
    wide = sub + 2 * RIM
    upper = sc[1] != 0
    for part in range(2):
        full[part, pl.ds(0, RIM), :] = jnp.where(upper, rim[part], 0.0)
        full[part, pl.ds(RIM, blk), :] = turned[part]
        full[part, pl.ds(RIM + blk, RIM), :] = jnp.where(upper, 0.0, rim[part])
    for part in range(2):
        own[part] = full[part, pl.ds(pl.multiple_of(sc[0] * sub, 8), wide), :]
        for k in range(1, GROUP):
            start = pl.multiple_of(jnp.bitwise_xor(sc[0], k) * sub, 8)
            for step in range(1, 4):
                target = outs[3 * (step - 1) + k - 1]
                for position, first, count in spans(plan[step]):
                    target[part, pl.ds(0, wide), lanes(position, count)] = full[
                        part, pl.ds(start, wide), lanes(first, count)
                    ]
                if step == 1:
                    for position, first, count in spans(plan[0]):
                        for at, row in ((wide, start), (wide + RIM, start + RIM + sub)):
                            target[part, pl.ds(at, RIM), lanes(position, count)] = full[
                                part, pl.ds(pl.multiple_of(row, 8), RIM), lanes(first, count)
                            ]


def raw_beams(plan, sub, own, low, high, remote, k, part, tile):
    wide = sub + 2 * RIM
    tiles = own.shape[2] // TILE
    if tile < 0:
        return low[k, part]
    if tile >= tiles:
        return high[k, part]
    if k == 0:
        return own[part, :, lanes(tile)]
    step = next(i for i in range(4) if tile in plan[i])
    at = plan[step].index(tile)
    if step > 0:
        return remote[step][k - 1][part, pl.ds(0, wide), lanes(at)]
    rims = remote[1][k - 1]
    return jnp.concatenate(
        [
            rims[part, pl.ds(wide, RIM), lanes(at)],
            remote[0][k - 1][part, :, lanes(at)],
            rims[part, pl.ds(wide + RIM, RIM), lanes(at)],
        ],
        axis=0,
    )


def edge_pack(plan, sub, own, *refs):
    remote = {0: refs[:3], 1: refs[3:6]}
    to_high, to_low = refs[6:]
    tiles = own.shape[2] // TILE
    for target, tile in ((to_high, tiles - 1), (to_low, 0)):
        for k in range(GROUP):
            for part in range(2):
                target[k, part] = raw_beams(plan, sub, own, None, None, remote, k, part, tile)


def spread(load, store_to, rows, table):
    coarse = table[FINE : FINE + 1, :]
    options = 2 * SPAN // COARSE + 1
    chosen = [coarse == float(i) for i in range(1, options)]
    step = 64
    for start in range(0, rows, step):
        size = min(step, rows - start)
        value = load(start, size)
        for i in range(1, options):
            value = jnp.where(chosen[i - 1], load(start + i * COARSE, size), value)
        store_to[pl.ds(start, size), :] = value


def fine_taps(shifted, start, size, table):
    total = None
    for tap in range(FINE):
        term = table[tap : tap + 1, :] * shifted[pl.ds(start + tap + 4, size), :]
        total = term if total is None else total + term
    return total


def split_into(lhs, at, size, value):
    high = value.astype(BF16)
    low = (value - high.astype(F32)).astype(BF16)
    lhs[pl.ds(at, size), pl.ds(0, TILE)] = high
    lhs[pl.ds(at, size), pl.ds(TILE, TILE)] = low


def turn_factor(base, fine, side, block, start, size):
    base_cos = base[side, 0, pl.ds(block, 1), :]
    base_sin = base[side, 1, pl.ds(block, 1), :]
    fine_cos = fine[side, 0, pl.ds(start, size), :]
    fine_sin = fine[side, 1, pl.ds(start, size), :]
    return base_cos * fine_cos - base_sin * fine_sin, base_sin * fine_cos + base_cos * fine_sin


def merge(plan, steps, runs, sub, has_edges, keep, sc, *refs):
    refs = list(refs)
    own = refs.pop(0)
    low = refs.pop(0) if has_edges else None
    high = refs.pop(0) if has_edges else None
    remote = {}
    for step in steps:
        remote[step] = refs[:3]
        del refs[:3]
    (taps_one, mats_one, lows_one, base_one, fine_one, taps_two, mats_two, base_two, fine_two) = refs[:9]
    del refs[:9]
    if keep:
        refs.pop(0)
    out, flat, shifted, shifted_two, lhs, lhs_two, mixed, mixed_two, parent, done, out_sem = refs
    tiles = own.shape[2] // TILE
    row_base, rows_total = sc[2], sc[3]
    wide = sub + 2 * RIM
    half = TILE // 2
    blank = jnp.zeros((half - wide, TILE), F32)
    results = []
    done_at = 0
    for first, count in runs:
        for i in range(count + 2):
            for side in range(2):
                for part in range(2):
                    pair = [
                        raw_beams(plan, sub, own, low, high, remote, 2 * side + j, part, first - 1 + i)
                        for j in range(2)
                    ]
                    flat[side, part, lanes(i), :] = jnp.concatenate(
                        [pair[0], blank, pair[1], blank], axis=0
                    ).T
        edges = first == 0 or first + count == tiles

        def parent_block(i, rows):
            for side in range(2):
                for part in range(2):

                    def load(start, size):
                        base = pl.multiple_of(i * TILE + TILE - 2 * HALO, 8)
                        return flat[side, part, pl.ds(base + start, size), :]

                    spread(load, shifted.at[side, part], rows + 16, taps_one[side])
                    for start in range(0, rows, min(rows, half)):
                        size = min(rows, half)
                        split_into(
                            lhs.at[side],
                            part * rows + start,
                            size,
                            fine_taps(shifted.at[side, part], start, size, taps_one[side]),
                        )
                both = pl.ds(0, 2 * rows)
                mixed[side, both, :] = jnp.dot(
                    lhs[side, both, :], mats_one[side], preferred_element_type=F32
                ) + jnp.dot(lhs[side, both, pl.ds(0, TILE)], lows_one[side], preferred_element_type=F32)
            size = min(rows, 32)
            for start in range(0, rows, size):
                sums = [[None, None], [None, None]]
                for side in range(2):
                    cosine, sine = turn_factor(base_one, fine_one, side, first + i, start, size)
                    if edges:
                        row = (
                            lax.broadcasted_iota(jnp.int32, (size, TILE), 0)
                            + row_base
                            + (first + i) * TILE
                            - HALO
                            + start
                        )
                        valid = jnp.logical_and(row >= 0, row < rows_total)
                        cosine = jnp.where(valid, cosine, 0.0)
                        sine = jnp.where(valid, sine, 0.0)
                    for image in range(2):
                        beams = pl.ds(image * TILE, TILE)
                        real = mixed[side, pl.ds(start, size), beams]
                        imag = mixed[side, pl.ds(rows + start, size), beams]
                        terms = (cosine * real - sine * imag, sine * real + cosine * imag)
                        for part in range(2):
                            have = sums[image][part]
                            sums[image][part] = terms[part] if have is None else have + terms[part]
                for image in range(2):
                    for part in range(2):
                        parent[image, part, pl.ds(pl.multiple_of(i * TILE + start, 8), size), :] = sums[
                            image
                        ][part]

        def final_block(i):
            for image in range(2):
                for part in range(2):

                    def load(start, size):
                        return parent[image, part, pl.ds(pl.multiple_of(i * TILE, 8) + start, size), :]

                    spread(load, shifted_two.at[image, part], TILE + 16, taps_two[image])
                    for start in range(0, TILE, half):
                        split_into(
                            lhs_two.at[image],
                            part * TILE + start,
                            half,
                            fine_taps(shifted_two.at[image, part], start, half, taps_two[image]),
                        )
                mixed_two[image] = jnp.dot(lhs_two[image], mats_two[image], preferred_element_type=F32)
            size = 32
            for start in range(0, TILE, size):
                sums = [None, None]
                for image in range(2):
                    cosine, sine = turn_factor(base_two, fine_two, image, first + i, start, size)
                    real, imag = (
                        mixed_two[image, pl.ds(part * TILE + start, size), pl.ds(0, TILE)]
                        + mixed_two[image, pl.ds(part * TILE + start, size), pl.ds(TILE, TILE)]
                        for part in range(2)
                    )
                    terms = (cosine * real - sine * imag, sine * real + cosine * imag)
                    for part in range(2):
                        sums[part] = terms[part] if sums[part] is None else sums[part] + terms[part]
                for part in range(2):
                    done[part, pl.ds(pl.multiple_of((done_at + i) * TILE + start, 8), size), :] = sums[part]

        parent_block(0, TILE)
        if count > 1:
            parent_block(1, TILE)

            def both(i, carry):
                final_block(i)
                parent_block(i + 2, TILE)
                return carry

            if count > 2:
                lax.fori_loop(0, count - 2, both, 0)
            final_block(count - 2)
        parent_block(count, 2 * HALO)
        final_block(count - 1)
        result = pltpu.make_async_copy(
            done.at[:, lanes(done_at, count), :], out.at[0, :, lanes(first, count), :], out_sem
        )
        result.start()
        results.append(result)
        done_at += count
    for result in results:
        result.wait()


def make_tables(
    sub,
    sc,
    shift_one,
    rtaps_one,
    bstart_one,
    btaps_one,
    prate_one,
    poff_one,
    shift_two,
    rtaps_two,
    bstart_two,
    btaps_two,
    prate_two,
    poff_two,
    taps_one,
    mats_one,
    lows_one,
    base_one,
    fine_one,
    taps_two,
    mats_two,
    base_two,
    fine_two,
):
    mine, beam, row_base = sc[0], sc[1], sc[2]
    total = sc[3].astype(F32)
    block = GROUP * beam + mine
    half = TILE // 2
    child_first = sub * block - RIM
    parent_first = 2 * sub * block - PRIM
    final_first = 4 * sub * block
    lane = lax.broadcasted_iota(jnp.int32, (TAPS, TILE), 1)

    def windowed(rows, first):
        count = rows.shape[1]
        moved = pltpu.roll(rows, lax.rem(2 * count - first, count), 1)[:, :TILE]
        spot = lane + first
        return jnp.where(jnp.logical_and(spot >= 0, spot < count), moved, jnp.zeros_like(moved))

    def line(table, side, first):
        return windowed(jnp.broadcast_to(table[pl.ds(side, 1), :], (TAPS, table.shape[1])), first)

    def twice(rows):
        return jnp.where(lane < half, rows, pltpu.roll(rows, half, 1))

    def range_table(target, shifts, taps):
        moved = shifts[0:1, :] + SPAN
        spot = lax.broadcasted_iota(jnp.int32, (2 * TAPS, TILE), 0)
        apart = spot - lax.rem(moved, jnp.int32(COARSE))
        total_rows = jnp.zeros((2 * TAPS, TILE), F32)
        for k in range(TAPS):
            total_rows = total_rows + jnp.where(apart == k, taps[k : k + 1, :], 0.0)
        target[...] = jnp.where(spot == FINE, (moved // COARSE).astype(F32), total_rows)

    def beam_matrix(starts, taps, first, height):
        apart = lax.broadcasted_iota(jnp.int32, (height, TILE), 0) - (starts[0:1, :] - first)
        matrix = jnp.zeros((height, TILE), F32)
        for k in range(TAPS):
            matrix = matrix + jnp.where(apart == k, taps[k : k + 1, :], 0.0)
        high = matrix.astype(BF16)
        return high, (matrix - high.astype(F32)).astype(BF16)

    def turn_tables(base, fine, rates, offsets, row_first):
        rate, offset = rates[0:1, :], offsets[0:1, :]
        blocks = base.shape[1]
        start = lax.broadcasted_iota(jnp.int32, (blocks, TILE), 0) * TILE + row_first
        angle = rate * (start.astype(F32) / total) + offset
        base[0] = jnp.cos(angle)
        base[1] = jnp.sin(angle)
        groups = TILE // 8
        coarse = rate * ((lax.broadcasted_iota(jnp.int32, (groups, TILE), 0) * 8).astype(F32) / total)
        small = rate * (lax.broadcasted_iota(jnp.int32, (8, TILE), 0).astype(F32) / total)
        coarse_cos, coarse_sin = jnp.cos(coarse), jnp.sin(coarse)
        small_cos, small_sin = jnp.cos(small), jnp.sin(small)
        for j in range(groups):
            cosine, sine = coarse_cos[j : j + 1, :], coarse_sin[j : j + 1, :]
            fine[0, pl.ds(8 * j, 8), :] = cosine * small_cos - sine * small_sin
            fine[1, pl.ds(8 * j, 8), :] = sine * small_cos + cosine * small_sin

    for slot in range(2):
        side = jnp.bitwise_xor(mine // 2, slot)
        range_table(
            taps_one.at[slot],
            twice(line(shift_one, side, child_first)),
            twice(windowed(rtaps_one[side], child_first)),
        )
        high, low = beam_matrix(
            line(bstart_one, side, parent_first),
            windowed(btaps_one[side], parent_first),
            child_first,
            half,
        )
        for target, value, copies in ((mats_one, high, 2), (lows_one, low, 1)):
            none = jnp.zeros_like(value)
            for i in range(copies):
                target[slot, pl.ds(i * TILE, half), pl.ds(0, TILE)] = value
                target[slot, pl.ds(i * TILE, half), pl.ds(TILE, TILE)] = none
                target[slot, pl.ds(i * TILE + half, half), pl.ds(0, TILE)] = none
                target[slot, pl.ds(i * TILE + half, half), pl.ds(TILE, TILE)] = value
        turn_tables(
            base_one.at[slot],
            fine_one.at[slot],
            line(prate_one, side, parent_first),
            line(poff_one, side, parent_first),
            row_base - HALO,
        )
        side = jnp.bitwise_xor(mine % 2, slot)
        range_table(
            taps_two.at[slot],
            line(shift_two, side, parent_first),
            windowed(rtaps_two[side], parent_first),
        )
        high, low = beam_matrix(
            line(bstart_two, side, final_first),
            windowed(btaps_two[side], final_first),
            parent_first,
            TILE,
        )
        mats_two[slot, pl.ds(0, TILE), pl.ds(0, TILE)] = high
        mats_two[slot, pl.ds(0, TILE), pl.ds(TILE, TILE)] = low
        mats_two[slot, pl.ds(TILE, TILE), pl.ds(0, TILE)] = high
        mats_two[slot, pl.ds(TILE, TILE), pl.ds(TILE, TILE)] = jnp.zeros_like(high)
        turn_tables(
            base_two.at[slot],
            fine_two.at[slot],
            line(prate_two, side, final_first),
            line(poff_two, side, final_first),
            row_base,
        )


def body(
    children,
    shift_one,
    rtaps_one,
    bstart_one,
    btaps_one,
    prate_one,
    poff_one,
    shift_two,
    rtaps_two,
    bstart_two,
    btaps_two,
    prate_two,
    poff_two,
):
    rows, blk = children.shape[2], children.shape[3]
    sub = blk // GROUP
    wide = sub + 2 * RIM
    tiles = rows // TILE
    apers, beams = lax.axis_size("aper"), lax.axis_size("beam")
    total = rows * lax.axis_size("rng")
    assert children.shape[0] == 1 and beams == 2 and apers % GROUP == 0
    assert blk == TILE and rows % (8 * TILE) == 0
    plan = plan_of(tiles)
    mine = lax.axis_index("aper") % GROUP
    beam = lax.axis_index("beam")
    row_base = lax.axis_index("rng") * rows
    sc = jnp.stack([mine, beam, row_base, jnp.int32(total)]).astype(jnp.int32)

    def out(*shape):
        return pltpu.VMEM(shape, F32)

    def near(arrays):
        return [pltpu.with_memory_space_constraint(array, pltpu.VMEM) for array in arrays]

    def call(kernel, *operands, **settings):
        return pl.pallas_call(kernel, compiler_params=PARAMS, **settings)(*operands)

    def swap(block, k):
        return lax.ppermute(block, "aper", [(i, i ^ k) for i in range(apers)])

    children = pltpu.with_memory_space_constraint(children, pltpu.HBM)
    widths = [len(part) * TILE for part in plan]
    *edge, rim, turned = call(
        functools.partial(first_pack, plan),
        sc,
        children,
        out_shape=[out(2, sub, widths[0])] * 3 + [out(2, RIM, rows), out(2, blk, rows)],
        in_specs=[SMEM, HBM],
        out_specs=[VMEM] * 5,
        scratch_shapes=[pltpu.VMEM((2, rows, blk), F32), pltpu.SemaphoreType.DMA((4,))],
    )
    remote = {0: [swap(edge[k - 1], k) for k in range(1, GROUP)]}
    rim = lax.ppermute(rim, "beam", [(0, 1), (1, 0)])
    *packed, own = call(
        functools.partial(second_pack, plan),
        sc, *near([turned, rim]),
        out_shape=[out(2, wide + 2 * RIM, widths[1])] * 3
        + [out(2, wide, widths[2])] * 3
        + [out(2, wide, widths[3])] * 3
        + [out(2, wide, rows)],
        in_specs=[SMEM, VMEM, VMEM],
        out_specs=[VMEM] * 10,
        scratch_shapes=[pltpu.VMEM((2, blk + 2 * RIM, rows), F32)],
    )
    for step in range(1, 4):
        remote[step] = [swap(packed[3 * (step - 1) + k - 1], k) for k in range(1, GROUP)]

    to_high, to_low = call(
        functools.partial(edge_pack, plan, sub),
        *near([own, *remote[0], *remote[1]]),
        out_shape=[out(GROUP, 2, wide, TILE)] * 2,
        in_specs=[VMEM] * 7,
        out_specs=[VMEM] * 2,
    )
    ranks = lax.axis_size("rng")
    low = lax.ppermute(to_high, "rng", [(i, i + 1) for i in range(ranks - 1)])
    high = lax.ppermute(to_low, "rng", [(i + 1, i) for i in range(ranks - 1)])

    def brief(*shape):
        return pltpu.VMEM(shape, BF16)

    blocks = tiles + 8
    given = (
        shift_one,
        rtaps_one,
        bstart_one,
        btaps_one,
        prate_one,
        poff_one,
        shift_two,
        rtaps_two,
        bstart_two,
        btaps_two,
        prate_two,
        poff_two,
    )
    tables = call(
        functools.partial(make_tables, sub),
        sc, *given,
        out_shape=[
            out(2, 2 * TAPS, TILE),
            brief(2, 2 * TILE, 2 * TILE),
            brief(2, TILE, 2 * TILE),
            out(2, 2, blocks, TILE),
            out(2, 2, TILE, TILE),
            out(2, 2 * TAPS, TILE),
            brief(2, 2 * TILE, 2 * TILE),
            out(2, 2, blocks, TILE),
            out(2, 2, TILE, TILE),
        ],
        in_specs=[SMEM] + [VMEM] * len(given),
        out_specs=[VMEM] * 9,
    )

    def merged(steps, runs, use_edges, before):
        arrays = [own] + ([low, high] if use_edges else [])
        for step in steps:
            arrays += remote[step]
        longest = max(count for _, count in runs)
        keep = before is not None
        operands = [sc, *near([*arrays, *tables])] + ([before] if keep else [])
        return call(
            functools.partial(merge, plan, steps, runs, sub, use_edges, keep),
            *operands,
            out_shape=jax.ShapeDtypeStruct((1, 2, rows, blk), F32),
            in_specs=[SMEM] + [VMEM] * (len(arrays) + len(tables)) + ([ANY] if keep else []),
            out_specs=ANY,
            input_output_aliases={len(operands) - 1: 0} if keep else {},
            scratch_shapes=[
                pltpu.VMEM((2, 2, (longest + 2) * TILE, TILE), F32),
                *[pltpu.VMEM((2, 2, TILE + 16, TILE), F32)] * 2,
                *[pltpu.VMEM((2, 2 * TILE, 2 * TILE), BF16)] * 2,
                *[pltpu.VMEM((2, 2 * TILE, 2 * TILE), F32)] * 2,
                pltpu.VMEM((2, 2, longest * TILE + 2 * HALO, TILE), F32),
                pltpu.VMEM((2, sum(count for _, count in runs) * TILE, TILE), F32),
                pltpu.SemaphoreType.DMA,
            ],
        )

    ready_one = plan[1][-1]
    ready_two = plan[2][-1]
    image = merged((0, 1), [(1, ready_one - 1)], False, None)
    image = merged(
        (0, 1, 2), [(tiles - 1, 1), (0, 1), (ready_one, ready_two - ready_one)], True, image
    )
    return merged((0, 1, 2, 3), [(ready_two, tiles - 1 - ready_two)], False, image)


def solution(mesh):
    return jax.shard_map(
        body,
        mesh=mesh,
        in_specs=(P("aper", None, "rng", "beam"),) + (P(),) * 12,
        out_specs=P("aper", None, "rng", "beam"),
        check_vma=False,
    )
```
